32 devices in a mesh: grp: 2 (over y), page: 16 (over z, x, core).
Axes of the slice: x: 2, y: 2, z: 4, core: 2. Of those that a mesh axis runs over, the one named last changes fastest.
Arguments:
- queries: bfloat16 [32, 4096], P('grp'), parts along dimension 0, may hold values from -64 to 64
- key_cache: bfloat16 [1024, 64, 1024], P(('grp', 'page')), parts along dimension 0, may hold values from -9 to 9
- value_cache: bfloat16 [1024, 64, 1024], P(('grp', 'page')), parts along dimension 0, may hold values from -16 to 16
- new_keys: bfloat16 [32, 1024], P('grp'), parts along dimension 0, may hold values from -16 to 16
- new_values: bfloat16 [32, 1024], P('grp'), parts along dimension 0, may hold values from -6 to 6
- chosen: int32 [16, 256], P('grp', 'page'), parts along dimension 0, may hold values from 0 to 511, as said below
Outputs:
- attended: bfloat16 [32, 4096], P('grp'), parts along dimension 0
The draws below stay inside these ranges and needn't reach their ends.
There are 2 independent parts, one for each index of `grp`. The reference program is written for one: setup_inputs(seed, part) draws one part's arguments, and reference() takes and returns one part's arrays. A program takes and returns all parts, laid end to end along the dimension named above; each array names one. Nothing has to cross between parts.
Inputs may be any that keep to these rules, and one draw needn't show every extreme that they name: `chosen`: each row names 256 different pages; at most 32 of a row's pages lie in the range of 32 pages of one device, and exactly 32 do for some device in every row.
All inputs are finite; a program needn't handle non-finite values.
Results may differ from the reference program's by a relative error of at most 0.004.
Values may be sent and summed in bfloat16 or wider, within the bound.
No kernel may reach another device: no remote copies, remote signals or barrier semaphores. Data moves between devices by JAX's collectives and lax.ppermute only.
A program may use at most 64 MiB of HBM per device.

```python
import jax
import jax.numpy as jnp
from jax import lax

MEMORY_GROUPS = 8
G = 4
D = 128
PAGE = 64
K = 256
PPD = 32
DRAFT = 16
CAPH = 32
N_PAGE = 16


def draw_chosen(key, part):
    overall_block_tally = PPD * N_PAGE
    key_order = jax.random.fold_in(key, 11)
    lookup_extra_rating = jax.random.fold_in(key, 12)
    key_heat = jax.random.fold_in(key, 13)
    precedence_rating = jax.vmap(lambda single: jax.random.permutation(single, overall_block_tally))(jax.random.split(key_order, MEMORY_GROUPS))
    precedence_rating = precedence_rating.astype(jnp.int32).reshape(MEMORY_GROUPS, N_PAGE, PPD)
    beaten = jnp.sum((precedence_rating[:, :, None, :] > precedence_rating[:, :, :, None]).astype(jnp.int32), axis=3)
    admissible_blocks = beaten < CAPH
    extra_lift_amount = jax.random.randint(lookup_extra_rating, (MEMORY_GROUPS, N_PAGE), 0, 4).astype(jnp.int32)
    strongest_blocks = jax.random.randint(key_heat, (MEMORY_GROUPS, 1), 0, N_PAGE).astype(jnp.int32)
    shard_identifiers = jnp.arange(N_PAGE, dtype=jnp.int32)[None, :]
    extra_lift_amount = jnp.where(shard_identifiers == strongest_blocks, 5, extra_lift_amount)
    block_ordering = jnp.where(admissible_blocks, extra_lift_amount[:, :, None] * overall_block_tally + precedence_rating, -1).reshape(MEMORY_GROUPS, overall_block_tally)
    picked = lax.top_k(block_ordering, K)[1]
    return picked.astype(jnp.int32)


def draw_queries(key, part):
    base = 2.0 * jax.random.normal(jax.random.fold_in(key, 21), (DRAFT, MEMORY_GROUPS * G, D), jnp.float32)
    return jnp.clip(base, -64.0, 64.0).reshape(DRAFT, MEMORY_GROUPS * G * D).astype(jnp.bfloat16)


def draw_key_cache(key, part):
    base = jax.random.normal(jax.random.fold_in(key, 31), (PPD * N_PAGE, PAGE, MEMORY_GROUPS * D), jnp.float32)
    return jnp.clip(base, -9.0, 9.0).astype(jnp.bfloat16)


def draw_value_cache(key, part):
    offsets = 1.5 * jax.random.normal(jax.random.fold_in(key, 41), (PPD * N_PAGE, 1, MEMORY_GROUPS * D), jnp.float32)
    noise = jax.random.normal(jax.random.fold_in(key, 42), (PPD * N_PAGE, PAGE, MEMORY_GROUPS * D), jnp.float32)
    return jnp.clip(noise + offsets, -16.0, 16.0).astype(jnp.bfloat16)


def bell_draw(rng, dims, scale, limit, kind=jnp.bfloat16):
    drawn = jax.random.normal(rng, dims, jnp.float32) * scale
    return jnp.minimum(jnp.maximum(drawn, -limit), limit).astype(kind)


def setup_inputs(seed: int = 0, part: int = 0) -> dict:
    seeds = jax.random.split(jax.random.key(seed), 7)
    part_splits = jax.random.split(jax.random.fold_in(seeds[6], part), 7)
    queries = draw_queries(jax.random.fold_in(jax.random.fold_in(seeds[6], part), 71), part)
    key_cache = draw_key_cache(jax.random.fold_in(jax.random.fold_in(seeds[6], part), 71), part)
    value_cache = draw_value_cache(jax.random.fold_in(jax.random.fold_in(seeds[6], part), 71), part)
    new_keys = bell_draw(part_splits[3], (DRAFT, MEMORY_GROUPS * D), 3.0, 16.0)
    new_values = bell_draw(part_splits[4], (DRAFT, MEMORY_GROUPS * D), 1.0, 6.0)
    chosen = draw_chosen(jax.random.fold_in(jax.random.fold_in(seeds[6], part), 71), part)
    return {"queries": queries, "key_cache": key_cache, "value_cache": value_cache, "new_keys": new_keys, "new_values": new_values, "chosen": chosen}


def reference(queries, key_cache, value_cache, new_keys, new_values, chosen):
    row_count = DRAFT * G
    scaling = D ** -0.5
    query_heads = queries.reshape(DRAFT, MEMORY_GROUPS, G, D).transpose(1, 0, 2, 3).reshape(MEMORY_GROUPS, row_count, D)
    key_fresh = new_keys.reshape(DRAFT, MEMORY_GROUPS, D).transpose(1, 0, 2)
    value_fresh = new_values.reshape(DRAFT, MEMORY_GROUPS, D).transpose(1, 0, 2)
    position = jnp.arange(row_count, dtype=jnp.int32) // G
    allowed = jnp.arange(DRAFT, dtype=jnp.int32)[None, :] <= position[:, None]

    def one_head(head_id):
        query_rows = query_heads[head_id]
        key_head = lax.dynamic_slice_in_dim(key_cache, head_id * D, D, 2)
        value_head = lax.dynamic_slice_in_dim(value_cache, head_id * D, D, 2)
        page_ids = chosen[head_id]
        key_rows = jnp.take(key_head, page_ids, axis=0).reshape(K * PAGE, D)
        value_rows = jnp.take(value_head, page_ids, axis=0).reshape(K * PAGE, D)
        cached = jnp.dot(query_rows, key_rows.T, preferred_element_type=jnp.float32) * scaling
        fresh_scores = jnp.dot(query_rows, key_fresh[head_id].T, preferred_element_type=jnp.float32) * scaling
        fresh_scores = jnp.where(allowed, fresh_scores, -jnp.inf)
        highest = jnp.maximum(jnp.max(cached, axis=1), jnp.max(fresh_scores, axis=1))
        weight_cached = jnp.exp(cached - highest[:, None]).astype(jnp.bfloat16)
        weight_fresh = jnp.where(allowed, jnp.exp(fresh_scores - highest[:, None]), 0.0).astype(jnp.bfloat16)
        totals = jnp.sum(weight_cached.astype(jnp.float32), axis=1) + jnp.sum(weight_fresh.astype(jnp.float32), axis=1)
        weighted = jnp.dot(weight_cached, value_rows, preferred_element_type=jnp.float32)
        weighted = weighted + jnp.dot(weight_fresh, value_fresh[head_id], preferred_element_type=jnp.float32)
        return (weighted / totals[:, None]).astype(jnp.bfloat16)

    attended = lax.map(one_head, jnp.arange(MEMORY_GROUPS, dtype=jnp.int32))
    return attended.reshape(MEMORY_GROUPS, DRAFT, G, D).transpose(1, 0, 2, 3).reshape(DRAFT, MEMORY_GROUPS * G * D)
```

```python
import jax
import jax.numpy as jnp
from jax import lax
from jax.experimental import pallas as pl
from jax.experimental.pallas import tpu as pltpu
from jax.sharding import PartitionSpec as P

ABSENT = -1e30
LOG2E = 1.4426950408889634
LANES = 128
STATS = 8


def vmem():
    return pl.BlockSpec(memory_space=pltpu.VMEM)


def spread_kernel(page_count, chosen_ref, wanted_ref):
    devices = wanted_ref.shape[0]
    kv_heads, listed = chosen_ref.shape
    chosen = chosen_ref[...]
    lane = lax.broadcasted_iota(jnp.int32, (kv_heads, LANES), 1)
    columns = [jnp.broadcast_to(chosen[:, j : j + 1], (kv_heads, LANES)) for j in range(listed)]

    def one_device(device, carry):
        page = jnp.where(lane < page_count, lane + device * page_count, -1)
        hit = columns[0] == page
        for column in columns[1:]:
            hit = jnp.logical_or(hit, column == page)
        own = jnp.logical_and(lane == page_count, device == 0)
        wanted_ref[device] = jnp.where(jnp.logical_or(hit, own), 1.0, 0.0)
        return carry

    lax.fori_loop(0, devices, one_device, 0)


def head_queries(queries_ref, head, groups):
    width = LANES
    return jnp.concatenate(
        [
            queries_ref[:, (head * groups + g) * width : (head * groups + g + 1) * width]
            for g in range(groups)
        ],
        axis=0,
    )


def padded_rows(rows):
    return jnp.concatenate(
        [rows, jnp.zeros((LANES - rows.shape[0], rows.shape[1]), rows.dtype)], axis=0
    )


def attend_kernel(
    wanted_ref, queries_ref, keys_ref, values_ref, new_keys_ref, new_values_ref, out_ref
):
    page_count, page_tokens, head_span = keys_ref.shape
    tokens = page_count * page_tokens
    kv_heads = wanted_ref.shape[1]
    drafts = queries_ref.shape[0]
    groups = queries_ref.shape[1] // head_span
    rows = drafts * groups
    devices, piece, width = out_ref.shape
    share = piece - STATS
    pieces = rows // share
    scale = width ** (-0.5) * LOG2E
    wanted = jnp.sum(wanted_ref[...], axis=0)
    bias = jnp.where(wanted > 0.5, 0.0, ABSENT)
    slot = lax.broadcasted_iota(jnp.int32, (LANES, tokens), 0)
    token_page = lax.broadcasted_iota(jnp.int32, (LANES, tokens), 1) // page_tokens
    expand = jnp.where(slot == token_page, 1.0, 0.0).astype(jnp.bfloat16)
    flags = jnp.where(wanted > 0.5, 1.0, 0.0).astype(jnp.bfloat16)
    token_flags = jnp.dot(flags, expand, preferred_element_type=jnp.float32)
    token_bias = jnp.where(token_flags > 0.5, 0.0, ABSENT)
    position = lax.broadcasted_iota(jnp.int32, (rows, LANES), 0) % drafts
    lane = lax.broadcasted_iota(jnp.int32, (rows, LANES), 1)
    causal = jnp.where(lane <= position, 0.0, ABSENT)
    stats = jnp.zeros((rows, LANES), jnp.float32)
    contract = (((1,), (1,)), ((), ()))
    for h in range(kv_heads):
        span = slice(h * width, (h + 1) * width)
        query_rows = head_queries(queries_ref, h, groups)
        keys = keys_ref[:, :, span].reshape(tokens, width)
        scores = lax.dot_general(query_rows, keys, contract, preferred_element_type=jnp.float32)
        scores = scores * scale + token_bias[h : h + 1, :]
        fresh = lax.dot_general(
            query_rows, padded_rows(new_keys_ref[:, span]), contract,
            preferred_element_type=jnp.float32,
        )
        fresh = fresh * scale + causal + bias[h : h + 1, page_count : page_count + 1]
        highest = jnp.maximum(
            jnp.max(scores, axis=1, keepdims=True), jnp.max(fresh, axis=1, keepdims=True)
        )
        present = highest > 0.5 * ABSENT
        offset = jnp.where(present, highest, 0.0).astype(jnp.bfloat16).astype(jnp.float32)
        weights = jnp.exp2(scores - offset).astype(jnp.bfloat16)
        fresh_weights = jnp.exp2(fresh - offset).astype(jnp.bfloat16)
        totals = jnp.sum(weights.astype(jnp.float32), axis=1, keepdims=True) + jnp.sum(
            fresh_weights.astype(jnp.float32), axis=1, keepdims=True
        )
        values = values_ref[:, :, span].reshape(tokens, width)
        weighted = jnp.dot(weights, values, preferred_element_type=jnp.float32)
        weighted = weighted + jnp.dot(
            fresh_weights, padded_rows(new_values_ref[:, span]), preferred_element_type=jnp.float32
        )
        weighted = weighted.astype(jnp.bfloat16)
        for i in range(pieces):
            out_ref[h * pieces + i, :share, :] = weighted[i * share : (i + 1) * share]
        coarse = totals.astype(jnp.bfloat16).astype(jnp.float32)
        level = jnp.where(present, offset, ABSENT)
        stats = jnp.where(lane == h * STATS, level, stats)
        stats = jnp.where(lane == h * STATS + 1, coarse, stats)
        stats = jnp.where(lane == h * STATS + 2, totals - coarse, stats)
    turned = padded_rows(stats).T
    for i in range(pieces):
        part = turned if i == 0 else pltpu.roll(turned, LANES - i * share, 1)
        part = part.astype(jnp.bfloat16)
        for h in range(kv_heads):
            out_ref[h * pieces + i, share:, :] = part[h * STATS : (h + 1) * STATS]


def merge_kernel(pieces_ref, out_ref):
    devices, piece, width = pieces_ref.shape
    share = piece - STATS
    stats = jnp.concatenate(
        [pieces_ref[d, share:, :].astype(jnp.float32) for d in range(devices)], axis=0
    )
    if devices * STATS < LANES:
        stats = jnp.concatenate(
            [stats, jnp.zeros((LANES - devices * STATS, width), jnp.float32)], axis=0
        )
    turned = stats.T[:share]
    levels = [turned[:, d * STATS : d * STATS + 1] for d in range(devices)]
    highest = levels[0]
    for level in levels[1:]:
        highest = jnp.maximum(highest, level)
    totals = jnp.zeros((share, 1), jnp.float32)
    weighted = jnp.zeros((share, width), jnp.float32)
    for d in range(devices):
        factor = jnp.exp2(levels[d] - highest)
        sums = (
            turned[:, d * STATS + 1 : d * STATS + 2] + turned[:, d * STATS + 2 : d * STATS + 3]
        )
        totals = totals + sums * factor
        weighted = weighted + pieces_ref[d, :share, :].astype(jnp.float32) * factor
    finished = (weighted / totals).astype(jnp.bfloat16)
    for d in range(devices):
        out_ref[d] = finished


def exchange(pieces):
    return lax.all_to_all(pieces, "page", split_axis=0, concat_axis=0, tiled=True)


def on_device(queries, key_cache, value_cache, new_keys, new_values, chosen):
    page_count, _, head_span = key_cache.shape
    kv_heads = chosen.shape[0]
    width = head_span // kv_heads
    drafts = queries.shape[0]
    groups = queries.shape[1] // head_span
    rows = drafts * groups
    devices = lax.axis_size("page")
    share = kv_heads * rows // devices
    f32 = jnp.float32
    bf16 = jnp.bfloat16
    limit = pltpu.CompilerParams(vmem_limit_bytes=24 * 1024 * 1024)

    wanted = pl.pallas_call(
        lambda *refs: spread_kernel(page_count, *refs),
        out_shape=jax.ShapeDtypeStruct((devices, kv_heads, LANES), f32),
        in_specs=[vmem()],
        out_specs=vmem(),
        compiler_params=limit,
        name="spread",
    )(chosen)
    wanted = exchange(wanted)
    pieces = pl.pallas_call(
        attend_kernel,
        out_shape=jax.ShapeDtypeStruct((devices, share + STATS, width), bf16),
        in_specs=[vmem()] * 6,
        out_specs=vmem(),
        compiler_params=limit,
        name="attend",
    )(wanted, queries, key_cache, value_cache, new_keys, new_values)
    pieces = exchange(pieces)
    finished = pl.pallas_call(
        merge_kernel,
        out_shape=jax.ShapeDtypeStruct((devices, share, width), bf16),
        in_specs=[vmem()],
        out_specs=vmem(),
        compiler_params=limit,
        name="merge",
    )(pieces)
    result = exchange(finished)
    return (
        result.reshape(kv_heads * groups, drafts, width)
        .transpose(1, 0, 2)
        .reshape(drafts, kv_heads * groups * width)
    )


def solution(mesh):
    placed = (
        P("grp", None),
        P(("grp", "page"), None, None),
        P(("grp", "page"), None, None),
        P("grp", None),
        P("grp", None),
        P("grp", "page"),
    )
    return jax.shard_map(
        on_device, mesh=mesh, in_specs=placed, out_specs=P("grp", None), check_vma=False
    )
```

```python
import jax
import jax.numpy as jnp
from jax import lax
from jax.experimental import pallas as pl
from jax.experimental.pallas import tpu as pltpu
from jax.sharding import PartitionSpec as P

ABSENT = -1e30
LOG2E = 1.4426950408889634
LANES = 128
STATS = 8
TILE = 8
RESIDENT_BYTES = 3 * 2**20


def vmem():
    return pl.BlockSpec(memory_space=pltpu.VMEM)


def hbm():
    return pl.BlockSpec(memory_space=pltpu.HBM)


def keep_in(space, *arrays):
    return [pltpu.with_memory_space_constraint(array, space) for array in arrays]


def spread_kernel(page_count, chosen_ref, wanted_ref):
    devices = wanted_ref.shape[0]
    kv_heads, listed = chosen_ref.shape
    chosen = chosen_ref[...]
    lane = lax.broadcasted_iota(jnp.int32, (kv_heads, LANES), 1)
    columns = [jnp.broadcast_to(chosen[:, j : j + 1], (kv_heads, LANES)) for j in range(listed)]

    def one_device(device, carry):
        page = jnp.where(lane < page_count, lane + device * page_count, -1)
        hit = columns[0] == page
        for column in columns[1:]:
            hit = jnp.logical_or(hit, column == page)
        own = jnp.logical_and(lane == page_count, device == 0)
        wanted_ref[device] = jnp.where(jnp.logical_or(hit, own), 1.0, 0.0)
        return carry

    lax.fori_loop(0, devices, one_device, 0)


def padded_rows(rows):
    return jnp.concatenate(
        [rows, jnp.zeros((LANES - rows.shape[0], rows.shape[1]), rows.dtype)], axis=0
    )


def score_kernel(
    groups, chunk, queries_hbm, new_keys_hbm, key_hbm,
    near_ref, far_hbm, fresh_ref,
    queries_ref, new_keys_ref, keys_ref, far_ref, small_sems, key_sems, far_sems,
):
    page_count, page_tokens, _ = key_hbm.shape
    resident, rows, tokens = near_ref.shape
    kv_heads = fresh_ref.shape[0]
    drafts = queries_hbm.shape[0]
    width = LANES
    scale = width ** (-0.5) * LOG2E
    small = [
        pltpu.make_async_copy(queries_hbm, queries_ref, small_sems.at[0]),
        pltpu.make_async_copy(new_keys_hbm, new_keys_ref, small_sems.at[1]),
    ]
    for copy in small:
        copy.start()
    key_copies = []
    for c in range(page_count // chunk):
        pages = pl.ds(c * chunk, chunk)
        copy = pltpu.make_async_copy(key_hbm.at[pages], keys_ref.at[pages], key_sems.at[c])
        copy.start()
        key_copies.append(copy)
    for copy in small:
        copy.wait()
    contract = (((1,), (1,)), ((), ()))
    query_heads = []
    for h in range(kv_heads):
        blocks = [
            queries_ref[t : t + TILE, (h * groups + g) * width : (h * groups + g + 1) * width]
            for t in range(0, drafts, TILE)
            for g in range(groups)
        ]
        query_heads.append(jnp.concatenate(blocks, axis=0))
        fresh_ref[h] = (
            lax.dot_general(
                query_heads[h], padded_rows(new_keys_ref[:, h * width : (h + 1) * width]),
                contract, preferred_element_type=jnp.float32,
            )
            * scale
        )
    span = chunk * page_tokens
    for c, copy in enumerate(key_copies):
        copy.wait()
        for h in range(kv_heads):
            keys = keys_ref[c * chunk : (c + 1) * chunk, :, h * width : (h + 1) * width]
            scores = lax.dot_general(
                query_heads[h], keys.reshape(span, width), contract,
                preferred_element_type=jnp.float32,
            )
            place = slice(c * span, (c + 1) * span)
            if h < resident:
                near_ref[h, :, place] = scores * scale
            else:
                far_ref[h - resident, :, place] = scores * scale
    far_copies = []
    for h in range(kv_heads - resident):
        copy = pltpu.make_async_copy(far_ref.at[h], far_hbm.at[h], far_sems.at[h])
        copy.start()
        far_copies.append(copy)
    for copy in far_copies:
        copy.wait()


def attend_kernel(
    drafts, groups, wanted_ref, near_ref, far_hbm, fresh_ref, value_hbm, new_values_hbm,
    out_ref,
    values_ref, far_ref, new_values_ref, value_sems, far_sems, small_sem,
):
    page_count, page_tokens, _ = value_hbm.shape
    resident, rows, tokens = near_ref.shape
    kv_heads = fresh_ref.shape[0]
    devices, piece, width = out_ref.shape
    share = piece - STATS
    pieces = rows // share
    small = pltpu.make_async_copy(new_values_hbm, new_values_ref, small_sem)
    value_copies = []
    far_copies = []
    for h in range(kv_heads):
        heads = pl.ds(h * width, width)
        copy = pltpu.make_async_copy(
            value_hbm.at[:, :, heads], values_ref.at[h], value_sems.at[h]
        )
        copy.start()
        value_copies.append(copy)
        if h == 0:
            small.start()
        if h >= resident:
            copy = pltpu.make_async_copy(
                far_hbm.at[h - resident], far_ref.at[h - resident], far_sems.at[h - resident]
            )
            copy.start()
            far_copies.append(copy)
    wanted = jnp.sum(wanted_ref[...], axis=0)
    bias = jnp.where(wanted > 0.5, 0.0, ABSENT)
    slot = lax.broadcasted_iota(jnp.int32, (LANES, tokens), 0)
    token_page = lax.broadcasted_iota(jnp.int32, (LANES, tokens), 1) // page_tokens
    expand = jnp.where(slot == token_page, 1.0, 0.0).astype(jnp.bfloat16)
    flags = jnp.where(wanted > 0.5, 1.0, 0.0).astype(jnp.bfloat16)
    token_flags = jnp.dot(flags, expand, preferred_element_type=jnp.float32)
    token_bias = jnp.where(token_flags > 0.5, 0.0, ABSENT)
    row = lax.broadcasted_iota(jnp.int32, (rows, LANES), 0)
    lane = lax.broadcasted_iota(jnp.int32, (rows, LANES), 1)
    position = row // (groups * TILE) * TILE + row % TILE
    causal = jnp.where(lane <= position, 0.0, ABSENT)
    stats = jnp.zeros((rows, LANES), jnp.float32)
    for h in range(kv_heads):
        if h >= resident:
            far_copies[h - resident].wait()
            scores = far_ref[h - resident]
        else:
            scores = near_ref[h]
        scores = scores + token_bias[h : h + 1, :]
        fresh = fresh_ref[h] + causal + bias[h : h + 1, page_count : page_count + 1]
        highest = jnp.maximum(
            jnp.max(scores, axis=1, keepdims=True), jnp.max(fresh, axis=1, keepdims=True)
        )
        present = highest > 0.5 * ABSENT
        offset = jnp.where(present, highest, 0.0).astype(jnp.bfloat16).astype(jnp.float32)
        weights = jnp.exp2(scores - offset).astype(jnp.bfloat16)
        fresh_weights = jnp.exp2(fresh - offset).astype(jnp.bfloat16)
        totals = jnp.sum(weights.astype(jnp.float32), axis=1, keepdims=True) + jnp.sum(
            fresh_weights.astype(jnp.float32), axis=1, keepdims=True
        )
        if h == 0:
            small.wait()
        value_copies[h].wait()
        values = values_ref[h].reshape(tokens, width)
        weighted = jnp.dot(weights, values, preferred_element_type=jnp.float32)
        weighted = weighted + jnp.dot(
            fresh_weights, padded_rows(new_values_ref[:, h * width : (h + 1) * width]),
            preferred_element_type=jnp.float32,
        )
        weighted = weighted.astype(jnp.bfloat16)
        for i in range(pieces):
            out_ref[i * kv_heads + h, :share, :] = weighted[i * share : (i + 1) * share]
        coarse = totals.astype(jnp.bfloat16).astype(jnp.float32)
        level = jnp.where(present, offset, ABSENT)
        stats = jnp.where(lane == h * STATS, level, stats)
        stats = jnp.where(lane == h * STATS + 1, coarse, stats)
        stats = jnp.where(lane == h * STATS + 2, totals - coarse, stats)
    turned = padded_rows(stats).T
    for i in range(pieces):
        part = turned if i == 0 else pltpu.roll(turned, LANES - i * share, 1)
        part = part.astype(jnp.bfloat16)
        for h in range(kv_heads):
            out_ref[i * kv_heads + h, share:, :] = part[h * STATS : (h + 1) * STATS]


def merge_kernel(pieces_ref, out_ref):
    devices, piece, width = pieces_ref.shape
    share = piece - STATS
    stats = jnp.concatenate(
        [pieces_ref[d, share:, :].astype(jnp.float32) for d in range(devices)], axis=0
    )
    if devices * STATS < LANES:
        stats = jnp.concatenate(
            [stats, jnp.zeros((LANES - devices * STATS, width), jnp.float32)], axis=0
        )
    turned = stats.T[:share]
    levels = [turned[:, d * STATS : d * STATS + 1] for d in range(devices)]
    highest = levels[0]
    for level in levels[1:]:
        highest = jnp.maximum(highest, level)
    totals = jnp.zeros((share, 1), jnp.float32)
    weighted = jnp.zeros((share, width), jnp.float32)
    for d in range(devices):
        factor = jnp.exp2(levels[d] - highest)
        sums = (
            turned[:, d * STATS + 1 : d * STATS + 2] + turned[:, d * STATS + 2 : d * STATS + 3]
        )
        totals = totals + sums * factor
        weighted = weighted + pieces_ref[d, :share, :].astype(jnp.float32) * factor
    finished = (weighted / totals).astype(jnp.bfloat16)
    for d in range(devices):
        out_ref[d] = finished


def exchange(pieces):
    return lax.all_to_all(pieces, "page", split_axis=0, concat_axis=0, tiled=True)


def on_device(queries, key_cache, value_cache, new_keys, new_values, chosen):
    page_count, page_tokens, head_span = key_cache.shape
    kv_heads = chosen.shape[0]
    width = head_span // kv_heads
    drafts = queries.shape[0]
    groups = queries.shape[1] // head_span
    rows = drafts * groups
    tokens = page_count * page_tokens
    devices = lax.axis_size("page")
    share = kv_heads * rows // devices
    chunk = 4
    resident = min(kv_heads - 1, RESIDENT_BYTES // (4 * rows * tokens))
    distant = kv_heads - resident
    f32 = jnp.float32
    bf16 = jnp.bfloat16
    dma = pltpu.SemaphoreType.DMA
    limit = pltpu.CompilerParams(vmem_limit_bytes=24 * 2**20)

    wanted = pl.pallas_call(
        lambda *refs: spread_kernel(page_count, *refs),
        out_shape=jax.ShapeDtypeStruct((devices, kv_heads, LANES), f32),
        in_specs=[vmem()],
        out_specs=vmem(),
        compiler_params=limit,
        name="spread",
    )(chosen)
    wanted = exchange(wanted)
    near, far, fresh = pl.pallas_call(
        lambda *refs: score_kernel(groups, chunk, *refs),
        out_shape=(
            pltpu.VMEM((resident, rows, tokens), f32),
            pltpu.HBM((distant, rows, tokens), f32),
            pltpu.VMEM((kv_heads, rows, LANES), f32),
        ),
        in_specs=[hbm()] * 3,
        out_specs=(vmem(), hbm(), vmem()),
        scratch_shapes=[
            pltpu.VMEM(queries.shape, bf16),
            pltpu.VMEM(new_keys.shape, bf16),
            pltpu.VMEM(key_cache.shape, bf16),
            pltpu.VMEM((distant, rows, tokens), f32),
            dma((2,)),
            dma((page_count // chunk,)),
            dma((distant,)),
        ],
        compiler_params=limit,
        cost_estimate=pl.CostEstimate(
            flops=2 * kv_heads * rows * tokens * width,
            bytes_accessed=2 * tokens * head_span,
            transcendentals=0,
        ),
        name="scores",
    )(*keep_in(pltpu.HBM, queries, new_keys, key_cache))
    far, value_cache, new_values = keep_in(pltpu.HBM, far, value_cache, new_values)
    wanted, near, fresh = keep_in(pltpu.VMEM, wanted, near, fresh)
    pieces = pl.pallas_call(
        lambda *refs: attend_kernel(drafts, groups, *refs),
        out_shape=jax.ShapeDtypeStruct((devices, share + STATS, width), bf16),
        in_specs=[vmem(), vmem(), hbm(), vmem(), hbm(), hbm()],
        out_specs=vmem(),
        scratch_shapes=[
            pltpu.VMEM((kv_heads, page_count, page_tokens, width), bf16),
            pltpu.VMEM((distant, rows, tokens), f32),
            pltpu.VMEM(new_values.shape, bf16),
            dma((kv_heads,)),
            dma((distant,)),
            dma,
        ],
        compiler_params=limit,
        name="attend",
    )(wanted, near, far, fresh, value_cache, new_values)
    pieces = exchange(pieces)
    finished = pl.pallas_call(
        merge_kernel,
        out_shape=jax.ShapeDtypeStruct((devices, share, width), bf16),
        in_specs=[vmem()],
        out_specs=vmem(),
        compiler_params=limit,
        name="merge",
    )(pieces)
    result = exchange(finished)
    return (
        result.reshape(drafts // TILE, kv_heads * groups, TILE, width)
        .transpose(0, 2, 1, 3)
        .reshape(drafts, kv_heads * groups * width)
    )


def solution(mesh):
    placed = (
        P("grp", None),
        P(("grp", "page"), None, None),
        P(("grp", "page"), None, None),
        P("grp", None),
        P("grp", None),
        P("grp", "page"),
    )
    return jax.shard_map(
        on_device, mesh=mesh, in_specs=placed, out_specs=P("grp", None), check_vma=False
    )
```

```python
import jax
import jax.numpy as jnp
from jax import lax
from jax.experimental import pallas as pl
from jax.experimental.pallas import tpu as pltpu
from jax.sharding import PartitionSpec as P

ABSENT = -1e30
LOG2E = 1.4426950408889634
LANES = 128
STATS = 8
TILE = 8
PAIR = 2


def vmem():
    return pl.BlockSpec(memory_space=pltpu.VMEM)


def hbm():
    return pl.BlockSpec(memory_space=pltpu.HBM)


def keep_in(space, *arrays):
    return [pltpu.with_memory_space_constraint(array, space) for array in arrays]


def padded_rows(rows):
    return jnp.concatenate(
        [rows, jnp.zeros((LANES - rows.shape[0], rows.shape[1]), rows.dtype)], axis=0
    )


def token_copies(source_hbm, target_ref, sem, pair, span):
    copies = []
    for tile in range(source_hbm.shape[1]):
        copies.append(
            pltpu.make_async_copy(
                source_hbm.at[:, tile, :, pl.ds(pair * span, span)],
                target_ref.at[pair, tile], sem.at[pair],
            )
        )
    return copies


def wait_all(target_ref, sem, pair):
    pltpu.make_async_copy(target_ref.at[pair], target_ref.at[pair], sem.at[pair]).wait()


def score_kernel(
    groups, queries_hbm, new_keys_hbm, new_values_hbm, key_hbm,
    weights_ref, peaks_ref, new_values_ref,
    queries_ref, rows_ref, new_keys_ref, keys_ref, scores_ref, small_sems, key_sems,
):
    page_count, tiles, _, _ = key_hbm.shape
    kv_heads, rows, _ = weights_ref.shape
    drafts = queries_hbm.shape[0]
    width = LANES
    span = PAIR * width
    scale = width ** (-0.5) * LOG2E
    lanes = page_count * TILE
    tokens = tiles * lanes
    small = [
        pltpu.make_async_copy(queries_hbm, queries_ref, small_sems.at[0]),
        pltpu.make_async_copy(new_keys_hbm, new_keys_ref, small_sems.at[1]),
    ]
    for copy in small:
        copy.start()
    pl.delay(16)
    for p in range(kv_heads // PAIR):
        for copy in token_copies(key_hbm, keys_ref, key_sems, p, span):
            copy.start()
    late = pltpu.make_async_copy(new_values_hbm, new_values_ref, small_sems.at[2])
    for copy in small:
        copy.wait()
    late.start()
    contract = (((1,), (1,)), ((), ()))
    row = lax.broadcasted_iota(jnp.int32, (rows, LANES), 0)
    column = lax.broadcasted_iota(jnp.int32, (rows, LANES), 1)
    causal = column <= row // (groups * TILE) * TILE + row % TILE
    for h in range(kv_heads):
        blocks = [
            queries_ref[t : t + TILE, (h * groups + g) * width : (h * groups + g + 1) * width]
            for t in range(0, drafts, TILE)
            for g in range(groups)
        ]
        query_rows = jnp.concatenate(blocks, axis=0)
        rows_ref[h] = query_rows
        fresh = scale * lax.dot_general(
            query_rows, padded_rows(new_keys_ref[:, h * width : (h + 1) * width]), contract,
            preferred_element_type=jnp.float32,
        )
        fresh = jnp.where(causal, fresh, ABSENT)
        peak = jnp.max(fresh, axis=1, keepdims=True)
        weights_ref[h, :, tokens:] = jnp.exp2(fresh - peak).astype(jnp.bfloat16)
        peaks_ref[h, :, lanes:] = jnp.broadcast_to(peak, (rows, LANES))

    lane = lax.broadcasted_iota(jnp.int32, (rows, lanes), 1)

    def score(h):
        query_rows = rows_ref[h]
        for tile in range(tiles):
            keys = keys_ref[h // PAIR, tile, :, :, h % PAIR * width : (h % PAIR + 1) * width]
            scores_ref[h, :, tile * lanes : (tile + 1) * lanes] = lax.dot_general(
                query_rows, keys.reshape(lanes, width), contract,
                preferred_element_type=jnp.float32,
            )

    def weigh(h):
        peak = scores_ref[h, :, :lanes]
        for tile in range(1, tiles):
            peak = jnp.maximum(peak, scores_ref[h, :, tile * lanes : (tile + 1) * lanes])
        step = 1
        while step < TILE:
            ahead = pltpu.roll(peak, lanes - step, 1)
            behind = pltpu.roll(peak, step, 1)
            peak = jnp.maximum(peak, jnp.where(lane // step % 2 == 0, ahead, behind))
            step *= 2
        peaks_ref[h, :, :lanes] = peak * scale
        for tile in range(tiles):
            place = slice(tile * lanes, (tile + 1) * lanes)
            weights = jnp.exp2((scores_ref[h, :, place] - peak) * scale)
            weights_ref[h, :, place] = weights.astype(jnp.bfloat16)

    for p in range(kv_heads // PAIR):
        wait_all(keys_ref, key_sems, p)
        for k in range(PAIR):
            score(p * PAIR + k)
            if p > 0:
                weigh((p - 1) * PAIR + k)
    late.wait()
    for k in range(PAIR):
        weigh(kv_heads - PAIR + k)


def attend_kernel(
    listed, me_ref, chosen_ref, weights_ref, peaks_ref, new_values_ref, value_hbm,
    out_ref,
    values_ref, scaled_ref, bias_ref, value_sems,
):
    page_count, tiles, _, _ = value_hbm.shape
    kv_heads, rows, _ = weights_ref.shape
    devices, piece, width = out_ref.shape
    share = piece - STATS
    pieces = rows // share
    span = PAIR * width
    pairs = kv_heads // PAIR
    lanes = page_count * TILE
    tokens = tiles * lanes
    for p in range(pairs):
        for copy in token_copies(value_hbm, values_ref, value_sems, p, span):
            copy.start()
    me = me_ref[0]
    target = me * page_count + lax.broadcasted_iota(jnp.int32, (kv_heads, lanes), 1) // TILE
    picked = target < 0
    for d in range(devices):
        chosen = chosen_ref[d]
        for j in range(listed):
            column = jnp.broadcast_to(chosen[:, j : j + 1], (kv_heads, lanes))
            picked = jnp.logical_or(picked, column == target)
    bias_ref[:, :lanes] = jnp.where(picked, 0.0, ABSENT)
    bias_ref[:, lanes:] = jnp.full((kv_heads, LANES), jnp.where(me == 0, 0.0, ABSENT))
    column = lax.broadcasted_iota(jnp.int32, (rows, LANES), 1)
    stats = [jnp.zeros((rows, LANES), jnp.float32)]

    def scale_head(h):
        level = peaks_ref[h] + bias_ref[h : h + 1, :]
        highest = jnp.max(level, axis=1, keepdims=True)
        present = highest > 0.5 * ABSENT
        factor = jnp.exp2(level - jnp.where(present, highest, 0.0)).astype(jnp.bfloat16)
        scaled = weights_ref[h, :, tokens:] * factor[:, lanes:]
        scaled_ref[h, :, tokens:] = scaled
        sums = scaled.astype(jnp.float32)
        for tile in range(tiles):
            place = slice(tile * lanes, (tile + 1) * lanes)
            scaled = weights_ref[h, :, place] * factor[:, :lanes]
            scaled_ref[h, :, place] = scaled
            scaled = scaled.astype(jnp.float32)
            for i in range(0, lanes, LANES):
                sums = sums + scaled[:, i : i + LANES]
        totals = jnp.sum(sums, axis=1, keepdims=True)
        top = jnp.where(present, highest, ABSENT)
        rest = [top, top, top, totals, totals]
        for k in range(5):
            part = rest[k].astype(jnp.bfloat16).astype(jnp.float32)
            stats[0] = jnp.where(column == h * STATS + k, part, stats[0])
            for later in range(k + 1, 3 if k < 3 else 5):
                rest[later] = rest[later] - part

    def product(p):
        values = values_ref[p].reshape(tokens, span)
        new_values = padded_rows(new_values_ref[:, p * span : (p + 1) * span])
        weights = scaled_ref[p * PAIR : (p + 1) * PAIR].reshape(PAIR * rows, tokens + LANES)
        half = tokens // 2
        weighted = jnp.dot(
            weights[:, :half], values[:half], preferred_element_type=jnp.float32
        ) + jnp.dot(
            weights[:, half:], jnp.concatenate([values[half:], new_values], axis=0),
            preferred_element_type=jnp.float32,
        )
        for k in range(PAIR):
            for i in range(pieces):
                first_row = k * rows + i * share
                out_ref[i * kv_heads + p * PAIR + k, :share, :] = weighted[
                    first_row : first_row + share, k * width : (k + 1) * width
                ].astype(jnp.bfloat16)

    for h in range(2 * PAIR):
        scale_head(h)
    for p in range(pairs):
        wait_all(values_ref, value_sems, p)
        product(p)
        if p + 2 < pairs:
            for k in range(PAIR):
                scale_head((p + 2) * PAIR + k)
    turned = padded_rows(stats[0]).T
    for i in range(pieces):
        part = turned if i == 0 else pltpu.roll(turned, LANES - i * share, 1)
        part = part.astype(jnp.bfloat16)
        for h in range(kv_heads):
            out_ref[i * kv_heads + h, share:, :] = part[h * STATS : (h + 1) * STATS]


def merge_kernel(pieces_ref, out_ref):
    devices, piece, width = pieces_ref.shape
    share = piece - STATS
    stats = jnp.concatenate(
        [pieces_ref[d, share:, :].astype(jnp.float32) for d in range(devices)], axis=0
    )
    if devices * STATS < LANES:
        stats = jnp.concatenate(
            [stats, jnp.zeros((LANES - devices * STATS, width), jnp.float32)], axis=0
        )
    turned = stats.T[:share]
    def stat(d, k):
        return turned[:, d * STATS + k : d * STATS + k + 1]

    levels = [stat(d, 0) + (stat(d, 1) + stat(d, 2)) for d in range(devices)]
    highest = levels[0]
    for level in levels[1:]:
        highest = jnp.maximum(highest, level)
    totals = jnp.zeros((share, 1), jnp.float32)
    weighted = jnp.zeros((share, width), jnp.float32)
    for d in range(devices):
        factor = jnp.exp2(levels[d] - highest)
        totals = totals + (stat(d, 3) + stat(d, 4)) * factor
        weighted = weighted + pieces_ref[d, :share, :].astype(jnp.float32) * factor
    finished = (weighted / totals).astype(jnp.bfloat16)
    for d in range(devices):
        out_ref[d] = finished


def exchange(pieces):
    return lax.all_to_all(pieces, "page", split_axis=0, concat_axis=0, tiled=True)


def on_device(queries, key_cache, value_cache, new_keys, new_values, chosen):
    page_count, page_tokens, head_span = key_cache.shape
    kv_heads, listed = chosen.shape
    width = head_span // kv_heads
    drafts = queries.shape[0]
    groups = queries.shape[1] // head_span
    rows = drafts * groups
    tokens = page_count * page_tokens
    tiles = page_tokens // TILE
    lanes = page_count * TILE
    pairs = kv_heads // PAIR
    span = PAIR * width
    devices = lax.axis_size("page")
    share = kv_heads * rows // devices
    f32 = jnp.float32
    bf16 = jnp.bfloat16
    dma = pltpu.SemaphoreType.DMA
    limit = pltpu.CompilerParams(vmem_limit_bytes=24 * 2**20)
    key_cache = key_cache.reshape(page_count, tiles, TILE, head_span)
    value_cache = value_cache.reshape(page_count, tiles, TILE, head_span)

    me = lax.axis_index("page").astype(jnp.int32).reshape(1)
    listing = jnp.pad(chosen, ((0, 0), (0, LANES - listed)), constant_values=-1)
    chosen_all = exchange(jnp.broadcast_to(listing[None], (devices,) + listing.shape))
    weights, peaks, new_values = pl.pallas_call(
        lambda *refs: score_kernel(groups, *refs),
        out_shape=(
            pltpu.VMEM((kv_heads, rows, tokens + LANES), bf16),
            pltpu.VMEM((kv_heads, rows, lanes + LANES), f32),
            pltpu.VMEM(new_values.shape, bf16),
        ),
        in_specs=[hbm()] * 4,
        out_specs=(vmem(), vmem(), vmem()),
        scratch_shapes=[
            pltpu.VMEM(queries.shape, bf16),
            pltpu.VMEM((kv_heads, rows, width), bf16),
            pltpu.VMEM(new_keys.shape, bf16),
            pltpu.VMEM((pairs, tiles, page_count, TILE, span), bf16),
            pltpu.VMEM((kv_heads, rows, tokens), f32),
            dma((3,)),
            dma((pairs,)),
        ],
        compiler_params=limit,
        cost_estimate=pl.CostEstimate(
            flops=2 * kv_heads * rows * tokens * width,
            bytes_accessed=2 * tokens * head_span,
            transcendentals=0,
        ),
        name="scores",
    )(*keep_in(pltpu.HBM, queries, new_keys, new_values, key_cache))
    value_cache, = keep_in(pltpu.HBM, value_cache)
    resting = keep_in(pltpu.VMEM, chosen_all, weights, peaks, new_values)
    pieces = pl.pallas_call(
        lambda *refs: attend_kernel(listed, *refs),
        out_shape=jax.ShapeDtypeStruct((devices, share + STATS, width), bf16),
        in_specs=[pl.BlockSpec(memory_space=pltpu.SMEM)] + [vmem()] * 4 + [hbm()],
        out_specs=vmem(),
        scratch_shapes=[
            pltpu.VMEM((pairs, tiles, page_count, TILE, span), bf16),
            pltpu.VMEM((kv_heads, rows, tokens + LANES), bf16),
            pltpu.VMEM((kv_heads, lanes + LANES), f32),
            dma((pairs,)),
        ],
        compiler_params=limit,
        name="attend",
    )(me, *resting, value_cache)
    pieces = exchange(pieces)
    finished = pl.pallas_call(
        merge_kernel,
        out_shape=jax.ShapeDtypeStruct((devices, share, width), bf16),
        in_specs=[vmem()],
        out_specs=vmem(),
        compiler_params=limit,
        name="merge",
    )(pieces)
    result = exchange(finished)
    return (
        result.reshape(drafts // TILE, kv_heads * groups, TILE, width)
        .transpose(0, 2, 1, 3)
        .reshape(drafts, kv_heads * groups * width)
    )


def solution(mesh):
    placed = (
        P("grp", None),
        P(("grp", "page"), None, None),
        P(("grp", "page"), None, None),
        P("grp", None),
        P("grp", None),
        P("grp", "page"),
    )
    return jax.shard_map(
        on_device, mesh=mesh, in_specs=placed, out_specs=P("grp", None), check_vma=False
    )
```

```python
import jax
import jax.numpy as jnp
from jax import lax
from jax.experimental import pallas as pl
from jax.experimental.pallas import tpu as pltpu
from jax.sharding import PartitionSpec as P

ABSENT = -1e30
LOG2E = 1.4426950408889634
LANES = 128
STATS = 8
TILE = 8
PAIR = 2


def vmem():
    return pl.BlockSpec(memory_space=pltpu.VMEM)


def hbm():
    return pl.BlockSpec(memory_space=pltpu.HBM)


def keep_in(space, *arrays):
    return [pltpu.with_memory_space_constraint(array, space) for array in arrays]


def padded_rows(rows):
    return jnp.concatenate(
        [rows, jnp.zeros((LANES - rows.shape[0], rows.shape[1]), rows.dtype)], axis=0
    )


def token_copies(source_hbm, target_ref, sem, pair, span):
    copies = []
    for tile in range(source_hbm.shape[1]):
        copies.append(
            pltpu.make_async_copy(
                source_hbm.at[:, tile, :, pl.ds(pair * span, span)],
                target_ref.at[pair, tile], sem.at[pair],
            )
        )
    return copies


def wait_all(target_ref, sem, pair):
    pltpu.make_async_copy(target_ref.at[pair], target_ref.at[pair], sem.at[pair]).wait()


def score_kernel(
    groups, queries_hbm, new_keys_hbm, new_values_hbm, key_hbm,
    weights_ref, peaks_ref, new_values_ref,
    queries_ref, rows_ref, new_keys_ref, keys_ref, scores_ref, small_sems, key_sems,
):
    page_count, tiles, _, _ = key_hbm.shape
    kv_heads, rows, _ = weights_ref.shape
    drafts = queries_hbm.shape[0]
    width = LANES
    span = PAIR * width
    scale = width ** (-0.5) * LOG2E
    lanes = page_count * TILE
    tokens = tiles * lanes
    small = [
        pltpu.make_async_copy(queries_hbm, queries_ref, small_sems.at[0]),
        pltpu.make_async_copy(new_keys_hbm, new_keys_ref, small_sems.at[1]),
    ]
    for copy in small:
        copy.start()
    pl.delay(16)
    for p in range(kv_heads // PAIR):
        for copy in token_copies(key_hbm, keys_ref, key_sems, p, span):
            copy.start()
    late = pltpu.make_async_copy(new_values_hbm, new_values_ref, small_sems.at[2])
    for copy in small:
        copy.wait()
    late.start()
    contract = (((1,), (1,)), ((), ()))
    row = lax.broadcasted_iota(jnp.int32, (rows, LANES), 0)
    column = lax.broadcasted_iota(jnp.int32, (rows, LANES), 1)
    causal = column <= row // (groups * TILE) * TILE + row % TILE
    for h in range(kv_heads):
        blocks = [
            queries_ref[t : t + TILE, (h * groups + g) * width : (h * groups + g + 1) * width]
            for t in range(0, drafts, TILE)
            for g in range(groups)
        ]
        query_rows = jnp.concatenate(blocks, axis=0)
        rows_ref[h] = query_rows
        fresh = scale * lax.dot_general(
            query_rows, padded_rows(new_keys_ref[:, h * width : (h + 1) * width]), contract,
            preferred_element_type=jnp.float32,
        )
        fresh = jnp.where(causal, fresh, ABSENT)
        peak = jnp.max(fresh, axis=1, keepdims=True)
        weights_ref[h, :, tokens:] = jnp.exp2(fresh - peak).astype(jnp.bfloat16)
        peaks_ref[h, :, lanes:] = jnp.broadcast_to(peak, (rows, LANES))

    lane = lax.broadcasted_iota(jnp.int32, (rows, lanes), 1)

    def score(h):
        query_rows = rows_ref[h]
        peak = None
        for tile in range(tiles):
            keys = keys_ref[h // PAIR, tile, :, :, h % PAIR * width : (h % PAIR + 1) * width]
            scores = lax.dot_general(
                query_rows, keys.reshape(lanes, width), contract,
                preferred_element_type=jnp.float32,
            )
            scores_ref[h, :, tile * lanes : (tile + 1) * lanes] = scores
            peak = scores if peak is None else jnp.maximum(peak, scores)
        peaks_ref[h, :, :lanes] = peak

    def weigh(h):
        peak = peaks_ref[h, :, :lanes]
        step = 1
        while step < TILE:
            ahead = pltpu.roll(peak, lanes - step, 1)
            behind = pltpu.roll(peak, step, 1)
            peak = jnp.maximum(peak, jnp.where(lane // step % 2 == 0, ahead, behind))
            step *= 2
        peaks_ref[h, :, :lanes] = peak * scale
        for tile in range(tiles):
            place = slice(tile * lanes, (tile + 1) * lanes)
            weights = jnp.exp2((scores_ref[h, :, place] - peak) * scale)
            weights_ref[h, :, place] = weights.astype(jnp.bfloat16)

    for p in range(kv_heads // PAIR):
        wait_all(keys_ref, key_sems, p)
        for k in range(PAIR):
            score(p * PAIR + k)
            if p > 0:
                weigh((p - 1) * PAIR + k)
    late.wait()
    for k in range(PAIR):
        weigh(kv_heads - PAIR + k)


def attend_kernel(
    listed, me_ref, chosen_ref, weights_ref, peaks_ref, new_values_ref, value_hbm,
    out_ref,
    values_ref, scaled_ref, bias_ref, value_sems,
):
    page_count, tiles, _, _ = value_hbm.shape
    kv_heads, rows, _ = weights_ref.shape
    devices, piece, width = out_ref.shape
    share = piece - STATS
    pieces = rows // share
    span = PAIR * width
    pairs = kv_heads // PAIR
    lanes = page_count * TILE
    tokens = tiles * lanes
    for p in range(pairs):
        for copy in token_copies(value_hbm, values_ref, value_sems, p, span):
            copy.start()
    me = me_ref[0]
    target = me * page_count + lax.broadcasted_iota(jnp.int32, (kv_heads, lanes), 1) // TILE
    picked = target < 0
    for d in range(devices):
        chosen = chosen_ref[d]
        for j in range(listed):
            column = jnp.broadcast_to(chosen[:, j : j + 1], (kv_heads, lanes))
            picked = jnp.logical_or(picked, column == target)
    bias_ref[:, :lanes] = jnp.where(picked, 0.0, ABSENT)
    bias_ref[:, lanes:] = jnp.full((kv_heads, LANES), jnp.where(me == 0, 0.0, ABSENT))
    column = lax.broadcasted_iota(jnp.int32, (rows, LANES), 1)
    stats = [jnp.zeros((rows, LANES), jnp.float32)]

    def scale_head(h):
        level = peaks_ref[h] + bias_ref[h : h + 1, :]
        highest = jnp.max(level, axis=1, keepdims=True)
        present = highest > 0.5 * ABSENT
        factor = jnp.exp2(level - jnp.where(present, highest, 0.0)).astype(jnp.bfloat16)
        scaled = weights_ref[h, :, tokens:] * factor[:, lanes:]
        scaled_ref[h, :, tokens:] = scaled
        sums = scaled.astype(jnp.float32)
        for tile in range(tiles):
            place = slice(tile * lanes, (tile + 1) * lanes)
            scaled = weights_ref[h, :, place] * factor[:, :lanes]
            scaled_ref[h, :, place] = scaled
            scaled = scaled.astype(jnp.float32)
            for i in range(0, lanes, LANES):
                sums = sums + scaled[:, i : i + LANES]
        totals = jnp.sum(sums, axis=1, keepdims=True)
        top = jnp.where(present, highest, ABSENT)
        rest = [top, top, top, totals, totals]
        for k in range(5):
            part = rest[k].astype(jnp.bfloat16).astype(jnp.float32)
            stats[0] = jnp.where(column == h * STATS + k, part, stats[0])
            for later in range(k + 1, 3 if k < 3 else 5):
                rest[later] = rest[later] - part

    def product(p):
        values = values_ref[p].reshape(tokens, span)
        new_values = padded_rows(new_values_ref[:, p * span : (p + 1) * span])
        weights = scaled_ref[p * PAIR : (p + 1) * PAIR].reshape(PAIR * rows, tokens + LANES)
        half = tokens // 2
        weighted = jnp.dot(
            weights[:, :half], values[:half], preferred_element_type=jnp.float32
        ) + jnp.dot(
            weights[:, half:], jnp.concatenate([values[half:], new_values], axis=0),
            preferred_element_type=jnp.float32,
        )
        for k in range(PAIR):
            for i in range(pieces):
                first_row = k * rows + i * share
                out_ref[i * kv_heads + p * PAIR + k, :share, :] = weighted[
                    first_row : first_row + share, k * width : (k + 1) * width
                ].astype(jnp.bfloat16)

    for h in range(2 * PAIR):
        scale_head(h)
    for p in range(0, pairs, 2):
        both = range(p, min(p + 2, pairs))
        for q in both:
            wait_all(values_ref, value_sems, q)
        for q in both:
            product(q)
        for h in range((p + 2) * PAIR, min((p + 4) * PAIR, kv_heads)):
            scale_head(h)
    turned = padded_rows(stats[0]).T
    for i in range(pieces):
        part = turned if i == 0 else pltpu.roll(turned, LANES - i * share, 1)
        part = part.astype(jnp.bfloat16)
        for h in range(kv_heads):
            out_ref[i * kv_heads + h, share:, :] = part[h * STATS : (h + 1) * STATS]


def merge_kernel(pieces_ref, out_ref):
    devices, piece, width = pieces_ref.shape
    share = piece - STATS

    def stat(k):
        return pieces_ref[:, share + k, :].astype(jnp.float32)

    level = stat(0) + (stat(1) + stat(2))
    factor = jnp.exp2(level - jnp.max(level, axis=0, keepdims=True))
    totals = jnp.sum((stat(3) + stat(4)) * factor, axis=0, keepdims=True)
    factor = factor / jnp.where(totals > 0.0, totals, 1.0)
    turned = padded_rows(factor).T[:share] if devices < LANES else factor.T[:share]
    weighted = jnp.zeros((share, width), jnp.float32)
    for d in range(devices):
        weighted = weighted + pieces_ref[d, :share, :].astype(jnp.float32) * turned[:, d : d + 1]
    finished = weighted.astype(jnp.bfloat16)
    for d in range(devices):
        out_ref[d] = finished


def exchange(pieces):
    return lax.all_to_all(pieces, "page", split_axis=0, concat_axis=0, tiled=True)


def on_device(queries, key_cache, value_cache, new_keys, new_values, chosen):
    page_count, page_tokens, head_span = key_cache.shape
    kv_heads, listed = chosen.shape
    width = head_span // kv_heads
    drafts = queries.shape[0]
    groups = queries.shape[1] // head_span
    rows = drafts * groups
    tokens = page_count * page_tokens
    tiles = page_tokens // TILE
    lanes = page_count * TILE
    pairs = kv_heads // PAIR
    span = PAIR * width
    devices = lax.axis_size("page")
    share = kv_heads * rows // devices
    f32 = jnp.float32
    bf16 = jnp.bfloat16
    dma = pltpu.SemaphoreType.DMA
    limit = pltpu.CompilerParams(vmem_limit_bytes=24 * 2**20)
    key_cache = key_cache.reshape(page_count, tiles, TILE, head_span)
    value_cache = value_cache.reshape(page_count, tiles, TILE, head_span)

    me = lax.axis_index("page").astype(jnp.int32).reshape(1)
    listing = jnp.pad(chosen, ((0, 0), (0, LANES - listed)), constant_values=-1)
    chosen_all = exchange(jnp.broadcast_to(listing[None], (devices,) + listing.shape))
    weights, peaks, new_values = pl.pallas_call(
        lambda *refs: score_kernel(groups, *refs),
        out_shape=(
            pltpu.VMEM((kv_heads, rows, tokens + LANES), bf16),
            pltpu.VMEM((kv_heads, rows, lanes + LANES), f32),
            pltpu.VMEM(new_values.shape, bf16),
        ),
        in_specs=[hbm()] * 4,
        out_specs=(vmem(), vmem(), vmem()),
        scratch_shapes=[
            pltpu.VMEM(queries.shape, bf16),
            pltpu.VMEM((kv_heads, rows, width), bf16),
            pltpu.VMEM(new_keys.shape, bf16),
            pltpu.VMEM((pairs, tiles, page_count, TILE, span), bf16),
            pltpu.VMEM((kv_heads, rows, tokens), f32),
            dma((3,)),
            dma((pairs,)),
        ],
        compiler_params=limit,
        cost_estimate=pl.CostEstimate(
            flops=2 * kv_heads * rows * tokens * width,
            bytes_accessed=2 * tokens * head_span,
            transcendentals=0,
        ),
        name="scores",
    )(*keep_in(pltpu.HBM, queries, new_keys, new_values, key_cache))
    value_cache, = keep_in(pltpu.HBM, value_cache)
    resting = keep_in(pltpu.VMEM, chosen_all, weights, peaks, new_values)
    pieces = pl.pallas_call(
        lambda *refs: attend_kernel(listed, *refs),
        out_shape=jax.ShapeDtypeStruct((devices, share + STATS, width), bf16),
        in_specs=[pl.BlockSpec(memory_space=pltpu.SMEM)] + [vmem()] * 4 + [hbm()],
        out_specs=vmem(),
        scratch_shapes=[
            pltpu.VMEM((pairs, tiles, page_count, TILE, span), bf16),
            pltpu.VMEM((kv_heads, rows, tokens + LANES), bf16),
            pltpu.VMEM((kv_heads, lanes + LANES), f32),
            dma((pairs,)),
        ],
        compiler_params=limit,
        name="attend",
    )(me, *resting, value_cache)
    pieces = exchange(pieces)
    finished = pl.pallas_call(
        merge_kernel,
        out_shape=jax.ShapeDtypeStruct((devices, share, width), bf16),
        in_specs=[vmem()],
        out_specs=vmem(),
        compiler_params=limit,
        name="merge",
    )(pieces)
    result = exchange(finished)
    return (
        result.reshape(drafts // TILE, kv_heads * groups, TILE, width)
        .transpose(0, 2, 1, 3)
        .reshape(drafts, kv_heads * groups * width)
    )


def solution(mesh):
    placed = (
        P("grp", None),
        P(("grp", "page"), None, None),
        P(("grp", "page"), None, None),
        P("grp", None),
        P("grp", None),
        P("grp", "page"),
    )
    return jax.shard_map(
        on_device, mesh=mesh, in_specs=placed, out_specs=P("grp", None), check_vma=False
    )
```

```python
import jax
import jax.numpy as jnp
from jax import lax
from jax.experimental import pallas as pl
from jax.experimental.pallas import tpu as pltpu
from jax.sharding import PartitionSpec as P

ABSENT = -1e30
LOG2E = 1.4426950408889634
LANES = 128
STATS = 8
TILE = 8
PAIR = 2


def vmem():
    return pl.BlockSpec(memory_space=pltpu.VMEM)


def hbm():
    return pl.BlockSpec(memory_space=pltpu.HBM)


def keep_in(space, *arrays):
    return [pltpu.with_memory_space_constraint(array, space) for array in arrays]


def padded_rows(rows):
    return jnp.concatenate(
        [rows, jnp.zeros((LANES - rows.shape[0], rows.shape[1]), rows.dtype)], axis=0
    )


def token_copies(source_hbm, target_ref, sem, pair, span):
    copies = []
    for tile in range(source_hbm.shape[1]):
        copies.append(
            pltpu.make_async_copy(
                source_hbm.at[:, tile, :, pl.ds(pair * span, span)],
                target_ref.at[pair, tile], sem.at[pair],
            )
        )
    return copies


def wait_all(target_ref, sem, pair):
    pltpu.make_async_copy(target_ref.at[pair], target_ref.at[pair], sem.at[pair]).wait()


def wait_part(target_ref, sem, pair, part):
    half = target_ref.shape[1] // 2
    place = target_ref.at[pair, pl.ds(part * half, half)]
    pltpu.make_async_copy(place, place, sem.at[2 * pair + part]).wait()


def score_kernel(
    groups, queries_hbm, new_keys_hbm, new_values_hbm, key_hbm,
    weights_ref, peaks_ref, new_values_ref,
    queries_ref, rows_ref, new_keys_ref, keys_ref, scores_ref, small_sems, key_sems,
):
    page_count, tiles, _, _ = key_hbm.shape
    kv_heads, rows, _ = weights_ref.shape
    drafts = queries_hbm.shape[0]
    width = LANES
    span = PAIR * width
    scale = width ** (-0.5) * LOG2E
    lanes = page_count * TILE
    tokens = tiles * lanes
    small = [
        pltpu.make_async_copy(queries_hbm, queries_ref, small_sems.at[0]),
        pltpu.make_async_copy(new_keys_hbm, new_keys_ref, small_sems.at[1]),
    ]
    for copy in small:
        copy.start()
    pl.delay(16)
    for p in range(kv_heads // PAIR):
        for copy in token_copies(key_hbm, keys_ref, key_sems, p, span):
            copy.start()
    late = pltpu.make_async_copy(new_values_hbm, new_values_ref, small_sems.at[2])
    for copy in small:
        copy.wait()
    late.start()
    contract = (((1,), (1,)), ((), ()))
    row = lax.broadcasted_iota(jnp.int32, (rows, LANES), 0)
    column = lax.broadcasted_iota(jnp.int32, (rows, LANES), 1)
    causal = column <= row // (groups * TILE) * TILE + row % TILE
    for h in range(kv_heads):
        blocks = [
            queries_ref[t : t + TILE, (h * groups + g) * width : (h * groups + g + 1) * width]
            for t in range(0, drafts, TILE)
            for g in range(groups)
        ]
        query_rows = jnp.concatenate(blocks, axis=0)
        rows_ref[h] = query_rows
        fresh = scale * lax.dot_general(
            query_rows, padded_rows(new_keys_ref[:, h * width : (h + 1) * width]), contract,
            preferred_element_type=jnp.float32,
        )
        fresh = jnp.where(causal, fresh, ABSENT)
        peak = jnp.max(fresh, axis=1, keepdims=True)
        weights_ref[h, :, tokens:] = jnp.exp2(fresh - peak).astype(jnp.bfloat16)
        peaks_ref[h, :, lanes:] = jnp.broadcast_to(peak, (rows, LANES))

    def score(h):
        query_rows = rows_ref[h]
        peak = None
        for tile in range(tiles):
            keys = keys_ref[h // PAIR, tile, :, :, h % PAIR * width : (h % PAIR + 1) * width]
            scores = lax.dot_general(
                query_rows, keys.reshape(lanes, width), contract,
                preferred_element_type=jnp.float32,
            )
            scores_ref[h, :, tile * lanes : (tile + 1) * lanes] = scores
            peak = scores if peak is None else jnp.maximum(peak, scores)
        peaks_ref[h, :, :lanes] = peak

    def weigh(h):
        peak = peaks_ref[h, :, :lanes]
        peaks_ref[h, :, :lanes] = peak * scale
        for tile in range(tiles):
            place = slice(tile * lanes, (tile + 1) * lanes)
            weights = jnp.exp2((scores_ref[h, :, place] - peak) * scale)
            weights_ref[h, :, place] = weights.astype(jnp.bfloat16)

    for p in range(kv_heads // PAIR):
        wait_all(keys_ref, key_sems, p)
        for k in range(PAIR):
            score(p * PAIR + k)
            if p > 0:
                weigh((p - 1) * PAIR + k)
    late.wait()
    for k in range(PAIR):
        weigh(kv_heads - PAIR + k)


def attend_kernel(
    listed, me_ref, chosen_ref, weights_ref, peaks_ref, new_values_ref, value_hbm,
    out_ref,
    values_ref, scaled_ref, bias_ref, sums_ref, value_sems,
):
    page_count, tiles, _, _ = value_hbm.shape
    kv_heads, rows, _ = weights_ref.shape
    devices, piece, width = out_ref.shape
    share = piece - STATS
    pieces = rows // share
    span = PAIR * width
    pairs = kv_heads // PAIR
    lanes = page_count * TILE
    tokens = tiles * lanes
    half_tiles = tiles // 2
    half = half_tiles * lanes
    for p in range(0, pairs, 2):
        for part in range(2):
            for q in range(p, min(p + 2, pairs)):
                for tile in range(part * half_tiles, (part + 1) * half_tiles):
                    pltpu.make_async_copy(
                        value_hbm.at[:, tile, :, pl.ds(q * span, span)],
                        values_ref.at[q, tile], value_sems.at[2 * q + part],
                    ).start()
    pl.delay(1)
    me = me_ref[0]
    target = me * page_count + lax.broadcasted_iota(jnp.int32, (kv_heads, lanes), 1) // TILE
    picked = target < 0
    for d in range(devices):
        chosen = chosen_ref[d]
        for j in range(listed):
            column = jnp.broadcast_to(chosen[:, j : j + 1], (kv_heads, lanes))
            picked = jnp.logical_or(picked, column == target)
    bias_ref[:, :lanes] = jnp.where(picked, 0.0, ABSENT)
    bias_ref[:, lanes:] = jnp.full((kv_heads, LANES), jnp.where(me == 0, 0.0, ABSENT))
    column = lax.broadcasted_iota(jnp.int32, (rows, LANES), 1)
    stats = [jnp.zeros((rows, LANES), jnp.float32)]

    def scale_head(h):
        level = peaks_ref[h] + bias_ref[h : h + 1, :]
        highest = jnp.max(level, axis=1, keepdims=True)
        present = highest > 0.5 * ABSENT
        factor = jnp.exp2(level - jnp.where(present, highest, 0.0)).astype(jnp.bfloat16)
        scaled = weights_ref[h, :, tokens:] * factor[:, lanes:]
        scaled_ref[h, :, tokens:] = scaled
        sums = scaled.astype(jnp.float32)
        for tile in range(tiles):
            place = slice(tile * lanes, (tile + 1) * lanes)
            scaled = weights_ref[h, :, place] * factor[:, :lanes]
            scaled_ref[h, :, place] = scaled
            scaled = scaled.astype(jnp.float32)
            for i in range(0, lanes, LANES):
                sums = sums + scaled[:, i : i + LANES]
        totals = jnp.sum(sums, axis=1, keepdims=True)
        top = jnp.where(present, highest, ABSENT)
        rest = [top, top, top, totals, totals]
        for k in range(5):
            part = rest[k].astype(jnp.bfloat16).astype(jnp.float32)
            stats[0] = jnp.where(column == h * STATS + k, part, stats[0])
            for later in range(k + 1, 3 if k < 3 else 5):
                rest[later] = rest[later] - part

    def product(p, part):
        place = slice(part * half, (part + 1) * half)
        values = values_ref[p, part * half_tiles : (part + 1) * half_tiles].reshape(half, span)
        weighted = jnp.dot(
            scaled_ref[p * PAIR : (p + 1) * PAIR, :, place].reshape(PAIR * rows, half), values,
            preferred_element_type=jnp.float32,
        )
        if part == 0:
            new_values = padded_rows(new_values_ref[:, p * span : (p + 1) * span])
            sums_ref[p] = weighted + jnp.dot(
                scaled_ref[p * PAIR : (p + 1) * PAIR, :, tokens:].reshape(PAIR * rows, LANES),
                new_values, preferred_element_type=jnp.float32,
            )
            return
        weighted = weighted + sums_ref[p]
        for k in range(PAIR):
            for i in range(pieces):
                first_row = k * rows + i * share
                out_ref[i * kv_heads + p * PAIR + k, :share, :] = weighted[
                    first_row : first_row + share, k * width : (k + 1) * width
                ].astype(jnp.bfloat16)

    for h in range(2 * PAIR):
        scale_head(h)
    for p in range(0, pairs, 2):
        both = range(p, min(p + 2, pairs))
        later = list(range((p + 2) * PAIR, min((p + 4) * PAIR, kv_heads)))
        for part in range(2):
            for q in both:
                wait_part(values_ref, value_sems, q, part)
            for q in both:
                product(q, part)
            for h in later[part::2]:
                scale_head(h)
    turned = padded_rows(stats[0]).T
    for i in range(pieces):
        part = turned if i == 0 else pltpu.roll(turned, LANES - i * share, 1)
        part = part.astype(jnp.bfloat16)
        for h in range(kv_heads):
            out_ref[i * kv_heads + h, share:, :] = part[h * STATS : (h + 1) * STATS]


def merge_kernel(pieces_ref, out_ref):
    devices, piece, width = pieces_ref.shape
    share = piece - STATS

    def stat(k):
        return pieces_ref[:, share + k, :].astype(jnp.float32)

    level = stat(0) + (stat(1) + stat(2))
    factor = jnp.exp2(level - jnp.max(level, axis=0, keepdims=True))
    totals = jnp.sum((stat(3) + stat(4)) * factor, axis=0, keepdims=True)
    factor = factor / jnp.where(totals > 0.0, totals, 1.0)
    turned = padded_rows(factor).T[:share] if devices < LANES else factor.T[:share]
    weighted = jnp.zeros((share, width), jnp.float32)
    for d in range(devices):
        weighted = weighted + pieces_ref[d, :share, :].astype(jnp.float32) * turned[:, d : d + 1]
    finished = weighted.astype(jnp.bfloat16)
    for d in range(devices):
        out_ref[d] = finished


def exchange(pieces):
    return lax.all_to_all(pieces, "page", split_axis=0, concat_axis=0, tiled=True)


def on_device(queries, key_cache, value_cache, new_keys, new_values, chosen):
    page_count, page_tokens, head_span = key_cache.shape
    kv_heads, listed = chosen.shape
    width = head_span // kv_heads
    drafts = queries.shape[0]
    groups = queries.shape[1] // head_span
    rows = drafts * groups
    tokens = page_count * page_tokens
    tiles = page_tokens // TILE
    lanes = page_count * TILE
    pairs = kv_heads // PAIR
    span = PAIR * width
    devices = lax.axis_size("page")
    share = kv_heads * rows // devices
    f32 = jnp.float32
    bf16 = jnp.bfloat16
    dma = pltpu.SemaphoreType.DMA
    limit = pltpu.CompilerParams(vmem_limit_bytes=24 * 2**20)
    key_cache = key_cache.reshape(page_count, tiles, TILE, head_span)
    value_cache = value_cache.reshape(page_count, tiles, TILE, head_span)

    me = lax.axis_index("page").astype(jnp.int32).reshape(1)
    listing = jnp.pad(chosen, ((0, 0), (0, LANES - listed)), constant_values=-1)
    chosen_all = exchange(jnp.broadcast_to(listing[None], (devices,) + listing.shape))
    weights, peaks, new_values = pl.pallas_call(
        lambda *refs: score_kernel(groups, *refs),
        out_shape=(
            pltpu.VMEM((kv_heads, rows, tokens + LANES), bf16),
            pltpu.VMEM((kv_heads, rows, lanes + LANES), f32),
            pltpu.VMEM(new_values.shape, bf16),
        ),
        in_specs=[hbm()] * 4,
        out_specs=(vmem(), vmem(), vmem()),
        scratch_shapes=[
            pltpu.VMEM(queries.shape, bf16),
            pltpu.VMEM((kv_heads, rows, width), bf16),
            pltpu.VMEM(new_keys.shape, bf16),
            pltpu.VMEM((pairs, tiles, page_count, TILE, span), bf16),
            pltpu.VMEM((kv_heads, rows, tokens), f32),
            dma((3,)),
            dma((pairs,)),
        ],
        compiler_params=limit,
        cost_estimate=pl.CostEstimate(
            flops=2 * kv_heads * rows * tokens * width,
            bytes_accessed=2 * tokens * head_span,
            transcendentals=0,
        ),
        name="scores",
    )(*keep_in(pltpu.HBM, queries, new_keys, new_values, key_cache))
    value_cache, = keep_in(pltpu.HBM, value_cache)
    resting = keep_in(pltpu.VMEM, chosen_all, weights, peaks, new_values)
    pieces = pl.pallas_call(
        lambda *refs: attend_kernel(listed, *refs),
        out_shape=jax.ShapeDtypeStruct((devices, share + STATS, width), bf16),
        in_specs=[pl.BlockSpec(memory_space=pltpu.SMEM)] + [vmem()] * 4 + [hbm()],
        out_specs=vmem(),
        scratch_shapes=[
            pltpu.VMEM((pairs, tiles, page_count, TILE, span), bf16),
            pltpu.VMEM((kv_heads, rows, tokens + LANES), bf16),
            pltpu.VMEM((kv_heads, lanes + LANES), f32),
            pltpu.VMEM((pairs, PAIR * rows, span), f32),
            dma((2 * pairs,)),
        ],
        compiler_params=limit,
        name="attend",
    )(me, *resting, value_cache)
    pieces = exchange(pieces)
    finished = pl.pallas_call(
        merge_kernel,
        out_shape=jax.ShapeDtypeStruct((devices, share, width), bf16),
        in_specs=[vmem()],
        out_specs=vmem(),
        compiler_params=limit,
        name="merge",
    )(pieces)
    result = exchange(finished)
    return (
        result.reshape(drafts // TILE, kv_heads * groups, TILE, width)
        .transpose(0, 2, 1, 3)
        .reshape(drafts, kv_heads * groups * width)
    )


def solution(mesh):
    placed = (
        P("grp", None),
        P(("grp", "page"), None, None),
        P(("grp", "page"), None, None),
        P("grp", None),
        P("grp", None),
        P("grp", "page"),
    )
    return jax.shard_map(
        on_device, mesh=mesh, in_specs=placed, out_specs=P("grp", None), check_vma=False
    )
```

```python
import jax
import jax.numpy as jnp
from jax import lax
from jax.experimental import pallas as pl
from jax.experimental.pallas import tpu as pltpu
from jax.sharding import PartitionSpec as P

ABSENT = -1e30
LOG2E = 1.4426950408889634
LANES = 128
STATS = 8
TILE = 8
PAIR = 2


def vmem():
    return pl.BlockSpec(memory_space=pltpu.VMEM)


def hbm():
    return pl.BlockSpec(memory_space=pltpu.HBM)


def keep_in(space, *arrays):
    return [pltpu.with_memory_space_constraint(array, space) for array in arrays]


def destination(head, part, kv_heads, share, block):
    tile, rest = divmod(part * share, block)
    return (tile * kv_heads * block + head * block + rest) // share


def padded_rows(rows):
    return jnp.concatenate(
        [rows, jnp.zeros((LANES - rows.shape[0], rows.shape[1]), rows.dtype)], axis=0
    )


def token_copies(source_hbm, target_ref, sem, pair, span):
    copies = []
    for tile in range(source_hbm.shape[1]):
        copies.append(
            pltpu.make_async_copy(
                source_hbm.at[:, tile, :, pl.ds(pair * span, span)],
                target_ref.at[pair, tile], sem.at[pair],
            )
        )
    return copies


def wait_all(target_ref, sem, pair):
    pltpu.make_async_copy(target_ref.at[pair], target_ref.at[pair], sem.at[pair]).wait()


def wait_part(target_ref, sem, pair, part):
    half = target_ref.shape[1] // 2
    place = target_ref.at[pair, pl.ds(part * half, half)]
    pltpu.make_async_copy(place, place, sem.at[2 * pair + part]).wait()


def score_kernel(
    groups, queries_hbm, new_keys_hbm, new_values_hbm, key_hbm,
    weights_ref, peaks_ref, new_values_ref,
    queries_ref, rows_ref, new_keys_ref, keys_ref, scores_ref, small_sems, key_sems,
):
    page_count, tiles, _, _ = key_hbm.shape
    kv_heads, rows, _ = weights_ref.shape
    drafts = queries_hbm.shape[0]
    width = LANES
    span = PAIR * width
    scale = width ** (-0.5) * LOG2E
    lanes = page_count * TILE
    tokens = tiles * lanes
    small = [
        pltpu.make_async_copy(queries_hbm, queries_ref, small_sems.at[0]),
        pltpu.make_async_copy(new_keys_hbm, new_keys_ref, small_sems.at[1]),
    ]
    for copy in small:
        copy.start()
    pl.delay(16)
    for p in range(kv_heads // PAIR):
        for copy in token_copies(key_hbm, keys_ref, key_sems, p, span):
            copy.start()
    late = pltpu.make_async_copy(new_values_hbm, new_values_ref, small_sems.at[2])
    for copy in small:
        copy.wait()
    late.start()
    contract = (((1,), (1,)), ((), ()))
    row = lax.broadcasted_iota(jnp.int32, (rows, LANES), 0)
    column = lax.broadcasted_iota(jnp.int32, (rows, LANES), 1)
    causal = column <= row // (groups * TILE) * TILE + row % TILE
    for h in range(kv_heads):
        blocks = [
            queries_ref[t : t + TILE, (h * groups + g) * width : (h * groups + g + 1) * width]
            for t in range(0, drafts, TILE)
            for g in range(groups)
        ]
        query_rows = jnp.concatenate(blocks, axis=0)
        rows_ref[h] = query_rows
        fresh = scale * lax.dot_general(
            query_rows, padded_rows(new_keys_ref[:, h * width : (h + 1) * width]), contract,
            preferred_element_type=jnp.float32,
        )
        fresh = jnp.where(causal, fresh, ABSENT)
        peak = jnp.max(fresh, axis=1, keepdims=True)
        weights_ref[h, :, tokens:] = jnp.exp2(fresh - peak).astype(jnp.bfloat16)
        peaks_ref[h, :, lanes:] = jnp.broadcast_to(peak, (rows, LANES))

    def score(h):
        query_rows = rows_ref[h]
        peak = None
        for tile in range(tiles):
            keys = keys_ref[h // PAIR, tile, :, :, h % PAIR * width : (h % PAIR + 1) * width]
            scores = lax.dot_general(
                query_rows, keys.reshape(lanes, width), contract,
                preferred_element_type=jnp.float32,
            )
            scores_ref[h, :, tile * lanes : (tile + 1) * lanes] = scores
            peak = scores if peak is None else jnp.maximum(peak, scores)
        peaks_ref[h, :, :lanes] = peak

    def weigh(h):
        peak = peaks_ref[h, :, :lanes]
        peaks_ref[h, :, :lanes] = peak * scale
        for tile in range(tiles):
            place = slice(tile * lanes, (tile + 1) * lanes)
            weights = jnp.exp2((scores_ref[h, :, place] - peak) * scale)
            weights_ref[h, :, place] = weights.astype(jnp.bfloat16)

    for p in range(kv_heads // PAIR):
        wait_all(keys_ref, key_sems, p)
        for k in range(PAIR):
            score(p * PAIR + k)
            if p > 0:
                weigh((p - 1) * PAIR + k)
    late.wait()
    for k in range(PAIR):
        weigh(kv_heads - PAIR + k)


def attend_kernel(
    listed, target, me_ref, chosen_ref, weights_ref, peaks_ref, new_values_ref, value_hbm,
    out_ref,
    values_ref, scaled_ref, bias_ref, sums_ref, value_sems,
):
    page_count, tiles, _, _ = value_hbm.shape
    kv_heads, rows, _ = weights_ref.shape
    devices, piece, width = out_ref.shape
    share = piece - STATS
    pieces = rows // share
    span = PAIR * width
    pairs = kv_heads // PAIR
    lanes = page_count * TILE
    tokens = tiles * lanes
    half_tiles = tiles // 2
    half = half_tiles * lanes
    for p in range(0, pairs, 2):
        for part in range(2):
            for q in range(p, min(p + 2, pairs)):
                for tile in range(part * half_tiles, (part + 1) * half_tiles):
                    pltpu.make_async_copy(
                        value_hbm.at[:, tile, :, pl.ds(q * span, span)],
                        values_ref.at[q, tile], value_sems.at[2 * q + part],
                    ).start()
    pl.delay(1)
    me = me_ref[0]
    page = me * page_count + lax.broadcasted_iota(jnp.int32, (kv_heads, lanes), 1) // TILE
    picked = page < 0
    for d in range(devices):
        chosen = chosen_ref[d]
        for j in range(listed):
            column = jnp.broadcast_to(chosen[:, j : j + 1], (kv_heads, lanes))
            picked = jnp.logical_or(picked, column == page)
    bias_ref[:, :lanes] = jnp.where(picked, 0.0, ABSENT)
    bias_ref[:, lanes:] = jnp.full((kv_heads, LANES), jnp.where(me == 0, 0.0, ABSENT))
    column = lax.broadcasted_iota(jnp.int32, (rows, LANES), 1)
    stats = [jnp.zeros((rows, LANES), jnp.float32)]

    def scale_head(h):
        level = peaks_ref[h] + bias_ref[h : h + 1, :]
        highest = jnp.max(level, axis=1, keepdims=True)
        present = highest > 0.5 * ABSENT
        factor = jnp.exp2(level - jnp.where(present, highest, 0.0)).astype(jnp.bfloat16)
        scaled = weights_ref[h, :, tokens:] * factor[:, lanes:]
        scaled_ref[h, :, tokens:] = scaled
        sums = scaled.astype(jnp.float32)
        for tile in range(tiles):
            place = slice(tile * lanes, (tile + 1) * lanes)
            scaled = weights_ref[h, :, place] * factor[:, :lanes]
            scaled_ref[h, :, place] = scaled
            scaled = scaled.astype(jnp.float32)
            for i in range(0, lanes, LANES):
                sums = sums + scaled[:, i : i + LANES]
        totals = jnp.sum(sums, axis=1, keepdims=True)
        top = jnp.where(present, highest, ABSENT)
        rest = [top, top, top, totals, totals]
        for k in range(5):
            part = rest[k].astype(jnp.bfloat16).astype(jnp.float32)
            stats[0] = jnp.where(column == h * STATS + k, part, stats[0])
            for later in range(k + 1, 3 if k < 3 else 5):
                rest[later] = rest[later] - part

    def product(p, part):
        place = slice(part * half, (part + 1) * half)
        values = values_ref[p, part * half_tiles : (part + 1) * half_tiles].reshape(half, span)
        weighted = jnp.dot(
            scaled_ref[p * PAIR : (p + 1) * PAIR, :, place].reshape(PAIR * rows, half), values,
            preferred_element_type=jnp.float32,
        )
        if part == 0:
            new_values = padded_rows(new_values_ref[:, p * span : (p + 1) * span])
            sums_ref[p] = weighted + jnp.dot(
                scaled_ref[p * PAIR : (p + 1) * PAIR, :, tokens:].reshape(PAIR * rows, LANES),
                new_values, preferred_element_type=jnp.float32,
            )
            return
        weighted = weighted + sums_ref[p]
        for k in range(PAIR):
            for i in range(pieces):
                first_row = k * rows + i * share
                out_ref[target(p * PAIR + k, i), :share, :] = weighted[
                    first_row : first_row + share, k * width : (k + 1) * width
                ].astype(jnp.bfloat16)

    for h in range(2 * PAIR):
        scale_head(h)
    for p in range(0, pairs, 2):
        both = range(p, min(p + 2, pairs))
        later = list(range((p + 2) * PAIR, min((p + 4) * PAIR, kv_heads)))
        for part in range(2):
            for q in both:
                wait_part(values_ref, value_sems, q, part)
            for q in both:
                product(q, part)
            for h in later[part::2]:
                scale_head(h)
    turned = padded_rows(stats[0]).T
    for i in range(pieces):
        part = turned if i == 0 else pltpu.roll(turned, LANES - i * share, 1)
        part = part.astype(jnp.bfloat16)
        for h in range(kv_heads):
            out_ref[target(h, i), share:, :] = part[h * STATS : (h + 1) * STATS]


def merge_kernel(pieces_ref, out_ref):
    devices, piece, width = pieces_ref.shape
    share = piece - STATS

    def stat(k):
        return pieces_ref[:, share + k, :].astype(jnp.float32)

    level = stat(0) + (stat(1) + stat(2))
    factor = jnp.exp2(level - jnp.max(level, axis=0, keepdims=True))
    totals = jnp.sum((stat(3) + stat(4)) * factor, axis=0, keepdims=True)
    factor = factor / jnp.where(totals > 0.0, totals, 1.0)
    turned = padded_rows(factor).T[:share] if devices < LANES else factor.T[:share]
    weighted = jnp.zeros((share, width), jnp.float32)
    for d in range(devices):
        weighted = weighted + pieces_ref[d, :share, :].astype(jnp.float32) * turned[:, d : d + 1]
    finished = weighted.astype(jnp.bfloat16)
    for d in range(devices):
        out_ref[d] = finished


def exchange(pieces):
    return lax.all_to_all(pieces, "page", split_axis=0, concat_axis=0, tiled=True)


def on_device(queries, key_cache, value_cache, new_keys, new_values, chosen):
    page_count, page_tokens, head_span = key_cache.shape
    kv_heads, listed = chosen.shape
    width = head_span // kv_heads
    drafts = queries.shape[0]
    groups = queries.shape[1] // head_span
    rows = drafts * groups
    tokens = page_count * page_tokens
    tiles = page_tokens // TILE
    lanes = page_count * TILE
    pairs = kv_heads // PAIR
    span = PAIR * width
    devices = lax.axis_size("page")
    share = kv_heads * rows // devices
    f32 = jnp.float32
    bf16 = jnp.bfloat16
    dma = pltpu.SemaphoreType.DMA
    limit = pltpu.CompilerParams(vmem_limit_bytes=24 * 2**20)
    key_cache = key_cache.reshape(page_count, tiles, TILE, head_span)
    value_cache = value_cache.reshape(page_count, tiles, TILE, head_span)

    block = groups * TILE

    def target(head, part):
        return destination(head, part, kv_heads, share, block)

    me = lax.axis_index("page").astype(jnp.int32).reshape(1)
    listing = jnp.pad(chosen, ((0, 0), (0, LANES - listed)), constant_values=-1)
    chosen_all = exchange(jnp.broadcast_to(listing[None], (devices,) + listing.shape))
    weights, peaks, new_values = pl.pallas_call(
        lambda *refs: score_kernel(groups, *refs),
        out_shape=(
            pltpu.VMEM((kv_heads, rows, tokens + LANES), bf16),
            pltpu.VMEM((kv_heads, rows, lanes + LANES), f32),
            pltpu.VMEM(new_values.shape, bf16),
        ),
        in_specs=[hbm()] * 4,
        out_specs=(vmem(), vmem(), vmem()),
        scratch_shapes=[
            pltpu.VMEM(queries.shape, bf16),
            pltpu.VMEM((kv_heads, rows, width), bf16),
            pltpu.VMEM(new_keys.shape, bf16),
            pltpu.VMEM((pairs, tiles, page_count, TILE, span), bf16),
            pltpu.VMEM((kv_heads, rows, tokens), f32),
            dma((3,)),
            dma((pairs,)),
        ],
        compiler_params=limit,
        cost_estimate=pl.CostEstimate(
            flops=2 * kv_heads * rows * tokens * width,
            bytes_accessed=2 * tokens * head_span,
            transcendentals=0,
        ),
        name="scores",
    )(*keep_in(pltpu.HBM, queries, new_keys, new_values, key_cache))
    value_cache, = keep_in(pltpu.HBM, value_cache)
    resting = keep_in(pltpu.VMEM, chosen_all, weights, peaks, new_values)
    pieces = pl.pallas_call(
        lambda *refs: attend_kernel(listed, target, *refs),
        out_shape=jax.ShapeDtypeStruct((devices, share + STATS, width), bf16),
        in_specs=[pl.BlockSpec(memory_space=pltpu.SMEM)] + [vmem()] * 4 + [hbm()],
        out_specs=vmem(),
        scratch_shapes=[
            pltpu.VMEM((pairs, tiles, page_count, TILE, span), bf16),
            pltpu.VMEM((kv_heads, rows, tokens + LANES), bf16),
            pltpu.VMEM((kv_heads, lanes + LANES), f32),
            pltpu.VMEM((pairs, PAIR * rows, span), f32),
            dma((2 * pairs,)),
        ],
        compiler_params=limit,
        name="attend",
    )(me, *resting, value_cache)
    pieces = exchange(pieces)
    finished = pl.pallas_call(
        merge_kernel,
        out_shape=jax.ShapeDtypeStruct((devices, share, width), bf16),
        in_specs=[vmem()],
        out_specs=vmem(),
        compiler_params=limit,
        name="merge",
    )(pieces)
    result = exchange(finished)
    return (
        result.reshape(drafts // TILE, kv_heads * groups, TILE, width)
        .transpose(0, 2, 1, 3)
        .reshape(drafts, kv_heads * groups * width)
    )


def solution(mesh):
    placed = (
        P("grp", None),
        P(("grp", "page"), None, None),
        P(("grp", "page"), None, None),
        P("grp", None),
        P("grp", None),
        P("grp", "page"),
    )
    return jax.shard_map(
        on_device, mesh=mesh, in_specs=placed, out_specs=P("grp", None), check_vma=False
    )
```

```python
import jax
import jax.numpy as jnp
from jax import lax
from jax.experimental import pallas as pl
from jax.experimental.pallas import tpu as pltpu
from jax.sharding import PartitionSpec as P

ABSENT = -1e30
LOG2E = 1.4426950408889634
LANES = 128
STATS = 8
TILE = 8
PAIR = 2


def vmem():
    return pl.BlockSpec(memory_space=pltpu.VMEM)


def hbm():
    return pl.BlockSpec(memory_space=pltpu.HBM)


def keep_in(space, *arrays):
    return [pltpu.with_memory_space_constraint(array, space) for array in arrays]


def destination(head, part, kv_heads, share, block):
    tile, rest = divmod(part * share, block)
    return (tile * kv_heads * block + head * block + rest) // share


def padded_rows(rows):
    return jnp.concatenate(
        [rows, jnp.zeros((LANES - rows.shape[0], rows.shape[1]), rows.dtype)], axis=0
    )


def token_copies(source_hbm, target_ref, sem, pair, span):
    copies = []
    for tile in range(source_hbm.shape[1]):
        copies.append(
            pltpu.make_async_copy(
                source_hbm.at[:, tile, :, pl.ds(pair * span, span)],
                target_ref.at[pair, tile], sem.at[pair],
            )
        )
    return copies


def wait_all(target_ref, sem, pair):
    pltpu.make_async_copy(target_ref.at[pair], target_ref.at[pair], sem.at[pair]).wait()


def wait_part(target_ref, sem, pair, part):
    half = target_ref.shape[1] // 2
    place = target_ref.at[pair, pl.ds(part * half, half)]
    pltpu.make_async_copy(place, place, sem.at[2 * pair + part]).wait()


def score_kernel(
    groups, queries_hbm, new_keys_hbm, new_values_hbm, key_hbm,
    weights_ref, peaks_ref, new_values_ref,
    queries_ref, rows_ref, new_keys_ref, keys_ref, scores_ref, small_sems, key_sems,
):
    page_count, tiles, _, _ = key_hbm.shape
    kv_heads, rows, _ = weights_ref.shape
    drafts = queries_hbm.shape[0]
    width = LANES
    span = PAIR * width
    scale = width ** (-0.5) * LOG2E
    lanes = page_count * TILE
    tokens = tiles * lanes
    small = [
        pltpu.make_async_copy(queries_hbm, queries_ref, small_sems.at[0]),
        pltpu.make_async_copy(new_keys_hbm, new_keys_ref, small_sems.at[1]),
    ]
    for copy in small:
        copy.start()
    pl.delay(16)
    for p in range(kv_heads // PAIR):
        for copy in token_copies(key_hbm, keys_ref, key_sems, p, span):
            copy.start()
    late = pltpu.make_async_copy(new_values_hbm, new_values_ref, small_sems.at[2])
    for copy in small:
        copy.wait()
    late.start()
    contract = (((1,), (1,)), ((), ()))
    row = lax.broadcasted_iota(jnp.int32, (rows, LANES), 0)
    column = lax.broadcasted_iota(jnp.int32, (rows, LANES), 1)
    causal = column <= row // (groups * TILE) * TILE + row % TILE
    for h in range(kv_heads):
        blocks = [
            queries_ref[t : t + TILE, (h * groups + g) * width : (h * groups + g + 1) * width]
            for t in range(0, drafts, TILE)
            for g in range(groups)
        ]
        query_rows = jnp.concatenate(blocks, axis=0)
        rows_ref[h] = query_rows
        fresh = scale * lax.dot_general(
            query_rows, padded_rows(new_keys_ref[:, h * width : (h + 1) * width]), contract,
            preferred_element_type=jnp.float32,
        )
        fresh = jnp.where(causal, fresh, ABSENT)
        peak = jnp.max(fresh, axis=1, keepdims=True)
        weights_ref[h, :, tokens:] = jnp.exp2(fresh - peak).astype(jnp.bfloat16)
        peaks_ref[h, :, lanes:] = jnp.broadcast_to(peak, (rows, LANES))

    def score(h):
        query_rows = rows_ref[h]
        peak = None
        for tile in range(tiles):
            keys = keys_ref[h // PAIR, tile, :, :, h % PAIR * width : (h % PAIR + 1) * width]
            scores = lax.dot_general(
                query_rows, keys.reshape(lanes, width), contract,
                preferred_element_type=jnp.float32,
            )
            scores_ref[h, :, tile * lanes : (tile + 1) * lanes] = scores
            peak = scores if peak is None else jnp.maximum(peak, scores)
        peaks_ref[h, :, :lanes] = peak

    def weigh(h):
        peak = peaks_ref[h, :, :lanes]
        peaks_ref[h, :, :lanes] = peak * scale
        for tile in range(tiles):
            place = slice(tile * lanes, (tile + 1) * lanes)
            weights = jnp.exp2((scores_ref[h, :, place] - peak) * scale)
            weights_ref[h, :, place] = weights.astype(jnp.bfloat16)

    for p in range(kv_heads // PAIR):
        wait_all(keys_ref, key_sems, p)
        for k in range(PAIR):
            score(p * PAIR + k)
            if p > 0:
                weigh((p - 1) * PAIR + k)
    late.wait()
    for k in range(PAIR):
        weigh(kv_heads - PAIR + k)


def attend_kernel(
    listed, target, me_ref, chosen_ref, weights_ref, peaks_ref, new_values_ref, value_hbm,
    out_ref,
    values_ref, scaled_ref, bias_ref, sums_ref, value_sems,
):
    page_count, tiles, _, _ = value_hbm.shape
    kv_heads, rows, _ = weights_ref.shape
    devices, piece, width = out_ref.shape
    share = piece - STATS
    pieces = rows // share
    span = PAIR * width
    pairs = kv_heads // PAIR
    lanes = page_count * TILE
    tokens = tiles * lanes
    half_tiles = tiles // 2
    half = half_tiles * lanes
    for p in range(0, pairs, 2):
        for part in range(2):
            for q in range(p, min(p + 2, pairs)):
                for tile in range(part * half_tiles, (part + 1) * half_tiles):
                    pltpu.make_async_copy(
                        value_hbm.at[:, tile, :, pl.ds(q * span, span)],
                        values_ref.at[q, tile], value_sems.at[2 * q + part],
                    ).start()
    pl.delay(1)
    me = me_ref[0]
    page = me * page_count + lax.broadcasted_iota(jnp.int32, (kv_heads, lanes), 1) // TILE
    picked = page < 0
    for d in range(devices):
        chosen = chosen_ref[d]
        for j in range(listed):
            column = jnp.broadcast_to(chosen[:, j : j + 1], (kv_heads, lanes))
            picked = jnp.logical_or(picked, column == page)
    bias_ref[:, :lanes] = jnp.where(picked, 0.0, ABSENT)
    bias_ref[:, lanes:] = jnp.full((kv_heads, LANES), jnp.where(me == 0, 0.0, ABSENT))
    column = lax.broadcasted_iota(jnp.int32, (rows, LANES), 1)
    stats = [jnp.zeros((rows, LANES), jnp.float32)]

    def scale_head(h):
        level = peaks_ref[h] + bias_ref[h : h + 1, :]
        highest = jnp.max(level, axis=1, keepdims=True)
        present = highest > 0.5 * ABSENT
        factor = jnp.exp2(level - jnp.where(present, highest, 0.0)).astype(jnp.bfloat16)
        scaled = weights_ref[h, :, tokens:] * factor[:, lanes:]
        scaled_ref[h, :, tokens:] = scaled
        sums = scaled.astype(jnp.float32)
        for tile in range(tiles):
            place = slice(tile * lanes, (tile + 1) * lanes)
            scaled = weights_ref[h, :, place] * factor[:, :lanes]
            scaled_ref[h, :, place] = scaled
            scaled = scaled.astype(jnp.float32)
            for i in range(0, lanes, LANES):
                sums = sums + scaled[:, i : i + LANES]
        totals = jnp.sum(sums, axis=1, keepdims=True)
        top = jnp.where(present, highest, ABSENT)
        rest = [top, top, top, totals, totals]
        for k in range(5):
            part = rest[k].astype(jnp.bfloat16).astype(jnp.float32)
            stats[0] = jnp.where(column == h * STATS + k, part, stats[0])
            for later in range(k + 1, 3 if k < 3 else 5):
                rest[later] = rest[later] - part

    def product(p, part):
        place = slice(part * half, (part + 1) * half)
        values = values_ref[p, part * half_tiles : (part + 1) * half_tiles].reshape(half, span)
        weighted = jnp.dot(
            scaled_ref[p * PAIR : (p + 1) * PAIR, :, place].reshape(PAIR * rows, half), values,
            preferred_element_type=jnp.float32,
        )
        if part == 0:
            new_values = padded_rows(new_values_ref[:, p * span : (p + 1) * span])
            sums_ref[p] = weighted + jnp.dot(
                scaled_ref[p * PAIR : (p + 1) * PAIR, :, tokens:].reshape(PAIR * rows, LANES),
                new_values, preferred_element_type=jnp.float32,
            )
            return
        weighted = weighted + sums_ref[p]
        for k in range(PAIR):
            for i in range(pieces):
                first_row = k * rows + i * share
                out_ref[target(p * PAIR + k, i), :share, :] = weighted[
                    first_row : first_row + share, k * width : (k + 1) * width
                ].astype(jnp.bfloat16)

    for h in range(2 * PAIR):
        scale_head(h)
    for p in range(0, pairs, 2):
        both = range(p, min(p + 2, pairs))
        later = list(range((p + 2) * PAIR, min((p + 4) * PAIR, kv_heads)))
        for part in range(2):
            for q in both:
                wait_part(values_ref, value_sems, q, part)
            for q in both:
                product(q, part)
            for h in later[part::2]:
                scale_head(h)
    turned = padded_rows(stats[0]).T
    for i in range(pieces):
        part = turned if i == 0 else pltpu.roll(turned, LANES - i * share, 1)
        part = part.astype(jnp.bfloat16)
        for h in range(kv_heads):
            out_ref[target(h, i), share:, :] = part[h * STATS : (h + 1) * STATS]


def merge_kernel(pieces_ref, out_ref):
    devices, piece, width = pieces_ref.shape
    share = piece - STATS

    def stat(k):
        return pieces_ref[:, share + k, :].astype(jnp.float32)

    level = stat(0) + (stat(1) + stat(2))
    factor = jnp.exp2(level - jnp.max(level, axis=0, keepdims=True))
    totals = jnp.sum((stat(3) + stat(4)) * factor, axis=0, keepdims=True)
    factor = factor / jnp.where(totals > 0.0, totals, 1.0)
    turned = padded_rows(factor).T[:share] if devices < LANES else factor.T[:share]
    weighted = jnp.zeros((share, width), jnp.float32)
    for d in range(devices):
        weighted = weighted + pieces_ref[d, :share, :].astype(jnp.float32) * turned[:, d : d + 1]
    finished = weighted.astype(jnp.bfloat16)
    for d in range(devices):
        out_ref[d] = finished


def exchange(pieces):
    return lax.all_to_all(pieces, "page", split_axis=0, concat_axis=0, tiled=True)


def on_device(queries, key_cache, value_cache, new_keys, new_values, chosen):
    page_count, page_tokens, head_span = key_cache.shape
    kv_heads, listed = chosen.shape
    width = head_span // kv_heads
    drafts = queries.shape[0]
    groups = queries.shape[1] // head_span
    rows = drafts * groups
    tokens = page_count * page_tokens
    tiles = page_tokens // TILE
    lanes = page_count * TILE
    pairs = kv_heads // PAIR
    span = PAIR * width
    devices = lax.axis_size("page")
    share = kv_heads * rows // devices
    f32 = jnp.float32
    bf16 = jnp.bfloat16
    dma = pltpu.SemaphoreType.DMA
    limit = pltpu.CompilerParams(vmem_limit_bytes=24 * 2**20)
    key_cache = key_cache.reshape(page_count, tiles, TILE, head_span)
    value_cache = value_cache.reshape(page_count, tiles, TILE, head_span)

    block = groups * TILE

    def target(head, part):
        return destination(head, part, kv_heads, share, block)

    me = lax.axis_index("page").astype(jnp.int32).reshape(1)
    listing = jnp.pad(chosen, ((0, 0), (0, LANES - listed)), constant_values=-1)
    chosen_all = exchange(jnp.broadcast_to(listing[None], (devices,) + listing.shape))
    weights, peaks, new_values = pl.pallas_call(
        lambda *refs: score_kernel(groups, *refs),
        out_shape=(
            pltpu.VMEM((kv_heads, rows, tokens + LANES), bf16),
            pltpu.VMEM((kv_heads, rows, lanes + LANES), f32),
            pltpu.VMEM(new_values.shape, bf16),
        ),
        in_specs=[hbm()] * 4,
        out_specs=(vmem(), vmem(), vmem()),
        scratch_shapes=[
            pltpu.VMEM(queries.shape, bf16),
            pltpu.VMEM((kv_heads, rows, width), bf16),
            pltpu.VMEM(new_keys.shape, bf16),
            pltpu.VMEM((pairs, tiles, page_count, TILE, span), bf16),
            pltpu.VMEM((kv_heads, rows, tokens), f32),
            dma((3,)),
            dma((pairs,)),
        ],
        compiler_params=limit,
        cost_estimate=pl.CostEstimate(
            flops=2 * kv_heads * rows * tokens * width,
            bytes_accessed=2 * tokens * head_span,
            transcendentals=0,
        ),
        name="scores",
    )(*keep_in(pltpu.HBM, queries, new_keys, new_values, key_cache))
    value_cache, = keep_in(pltpu.HBM, value_cache)
    resting = keep_in(pltpu.VMEM, chosen_all, weights, peaks, new_values)
    pieces = pl.pallas_call(
        lambda *refs: attend_kernel(listed, target, *refs),
        out_shape=jax.ShapeDtypeStruct((devices, share + STATS, width), bf16),
        in_specs=[pl.BlockSpec(memory_space=pltpu.SMEM)] + [vmem()] * 4 + [hbm()],
        out_specs=vmem(),
        scratch_shapes=[
            pltpu.VMEM((pairs, tiles, page_count, TILE, span), bf16),
            pltpu.VMEM((kv_heads, rows, tokens + LANES), bf16),
            pltpu.VMEM((kv_heads, lanes + LANES), f32),
            pltpu.VMEM((pairs, PAIR * rows, span), f32),
            dma((2 * pairs,)),
        ],
        compiler_params=pltpu.CompilerParams(
            vmem_limit_bytes=24 * 2**20
        ),
        name="attend",
    )(me, *resting, value_cache)
    pieces = exchange(pieces)
    finished = pl.pallas_call(
        merge_kernel,
        out_shape=jax.ShapeDtypeStruct((devices, share, width), bf16),
        in_specs=[vmem()],
        out_specs=vmem(),
        compiler_params=limit,
        name="merge",
    )(pieces)
    result = exchange(finished)
    return (
        result.reshape(drafts // TILE, kv_heads * groups, TILE, width)
        .transpose(0, 2, 1, 3)
        .reshape(drafts, kv_heads * groups * width)
    )


def solution(mesh):
    placed = (
        P("grp", None),
        P(("grp", "page"), None, None),
        P(("grp", "page"), None, None),
        P("grp", None),
        P("grp", None),
        P("grp", "page"),
    )
    return jax.shard_map(
        on_device, mesh=mesh, in_specs=placed, out_specs=P("grp", None), check_vma=False
    )
```
